256 devices in a mesh: dp: 64 (over z, y, core), mp: 4 (over x).
Axes of the slice: x: 4, y: 4, z: 8, core: 2. Of those that a mesh axis runs over, the one named last changes fastest.
Arguments:
- tokens: bfloat16 [393216, 512], P('dp'), may hold values from -6 to 6
- w_uvqk: bfloat16 [512, 2048], P(None, 'mp')
- w_out: bfloat16 [512, 512], replicated, may hold values from -0.25 to 0.25
- hist_len: int32 [64, 24], P('dp'), may hold values from 64 to 256, as said below
- owner: int32 [64, 24], P('dp'), may hold values from 0 to 63, as said below
- recv_offset: int32 [64, 24], P('dp'), may hold values from 0 to 47, as said below
- block_start: int32 [64, 24], P('dp'), may hold values from 0 to 47, as said below
Outputs:
- packed_out: bfloat16 [393216, 512], P('dp', 'mp')
- user_state: bfloat16 [1536, 512], P('dp', 'mp')
The draws below stay inside these ranges and needn't reach their ends.
Inputs may be any that keep to these rules, and one draw needn't show every extreme that they name: User (d, u) has ceil(hist_len / 128) blocks, at most 2. owner[d, u] = (p(d) + r(u mod 64)) mod 64 for two permutations p, r of the indices of dp drawn from the seed: every owner receives exactly 24 users, and one device sends at most 1 users to one owner. On some owner every received user has 2 blocks. `recv_offset`: the users of one owner occupy disjoint runs of its 48 blocks, in the order of u; on some owner they fill all 48 blocks. `block_start`: the users of one device occupy disjoint runs of its 48 blocks, in the order of u.
All inputs are finite; a program needn't handle non-finite values.
Results may differ from the reference program's by a relative error of at most 0.0059.
Values may be sent and summed in bfloat16 or wider, within the bound.
A program may use at most 128 MiB of HBM per device.

```python
import jax
import jax.numpy as jnp
from jax import lax

D = 512
HEADS = 4
BLOCK = 128
MAXB = 2
USERS_DEV = 24
BLK_DEV = 48
ROWS = 393216
N_DP = 64


def place_runs(key, run_sizes, salt_value):
    before = jnp.cumsum(run_sizes, axis=1) - run_sizes
    spare_blocks = BLK_DEV - jnp.sum(run_sizes, axis=1, keepdims=True)
    gap_sums = jnp.cumsum(jax.random.randint(jax.random.fold_in(key, salt_value), run_sizes.shape, 0, 2), axis=1)
    return (before + jnp.minimum(gap_sums, spare_blocks)).astype(jnp.int32)


def draw_tables(key):
    device_count = N_DP
    user_count = USERS_DEV
    dev_perm = jax.random.permutation(jax.random.fold_in(key, 101), device_count).astype(jnp.int32)
    user_perm = jax.random.permutation(jax.random.fold_in(key, 102), device_count).astype(jnp.int32)
    user_ids = jnp.arange(user_count, dtype=jnp.int32)
    shifts = user_perm[user_ids % device_count]
    owners = ((dev_perm[:, None] + shifts[None, :]) % device_count).astype(jnp.int32)
    hottest = jax.random.randint(jax.random.fold_in(key, 103), (), 0, device_count)
    coin_flip = jax.random.randint(jax.random.fold_in(key, 104), (device_count, user_count), 0, 4)
    small_count = jax.random.randint(jax.random.fold_in(key, 108), (device_count, user_count), 1, MAXB + 1)
    counts = jnp.where(coin_flip > 0, MAXB, small_count)
    counts = jnp.where(owners == hottest, MAXB, counts).astype(jnp.int32)
    least_tail = jnp.where(counts == 1, BLOCK // 2, 1)
    extra_rows = jax.random.randint(jax.random.fold_in(key, 105), (device_count, user_count), 0, BLOCK + 1)
    last_fill = least_tail + extra_rows % (BLOCK + 1 - least_tail)
    lengths = ((counts - 1) * BLOCK + last_fill).astype(jnp.int32)
    starts = place_runs(key, counts, 106)
    inverse = jnp.zeros((device_count,), jnp.int32).at[dev_perm].set(jnp.arange(device_count, dtype=jnp.int32))
    sources = inverse[(jnp.arange(device_count, dtype=jnp.int32)[:, None] - shifts[None, :]) % device_count]
    incoming = counts[sources, user_ids[None, :]]
    landing = place_runs(key, incoming, 107)
    offsets = landing[owners, user_ids[None, :]].astype(jnp.int32)
    return (lengths, owners, offsets, starts)


def draw_hist_len(key, part):
    return draw_tables(key)[0]


def draw_owner(key, part):
    return draw_tables(key)[1]


def draw_recv_offset(key, part):
    return draw_tables(key)[2]


def draw_block_start(key, part):
    return draw_tables(key)[3]


def draw_w_uvqk(key, part):
    base_draw = jax.random.normal(jax.random.fold_in(key, 1), (D, 4 * D), jnp.float32)
    log_scale = jax.random.uniform(jax.random.fold_in(key, 2), (1, 4 * D), jnp.float32, -1.2, 1.2)
    return (base_draw * jnp.exp(log_scale) / jnp.sqrt(D * 1.0)).astype(jnp.bfloat16)


def shard_levels(rng, extent, split, least, high):
    factor_of = 1.0
    for dim, parts in split:
        steps = jax.random.uniform(jax.random.fold_in(jax.random.fold_in(rng, 6), dim), (parts,), jnp.float32, least / len(split), high / len(split))
        factor_of = factor_of * jnp.repeat(jnp.exp(steps), extent[dim] // parts).reshape((-1,) + (1,) * (len(extent) - 1 - dim))
    return factor_of


def normal_values(key, extent, spread, bound, split=(), held_as=jnp.bfloat16):
    values = jax.random.normal(key, extent, jnp.float32) * spread
    if len(split) > 0:
        values = shard_levels(key, extent, split, -0.22, 0.18) * values
    return jnp.clip(values, min=-bound, max=bound).astype(held_as)


def setup_inputs(seed: int = 0) -> dict:
    key_of = jax.random.split(jax.random.key(seed), 8)
    tokens = normal_values(key_of[0], (ROWS, D), 1.0, 6.0, ((0, 64),))
    w_uvqk = draw_w_uvqk(jax.random.fold_in(key_of[7], 71), 0)
    w_out = normal_values(key_of[2], (D, D), D ** -0.5, 0.25)
    hist_len = draw_hist_len(jax.random.fold_in(key_of[7], 71), 0)
    owner = draw_owner(jax.random.fold_in(key_of[7], 71), 0)
    recv_offset = draw_recv_offset(jax.random.fold_in(key_of[7], 71), 0)
    block_start = draw_block_start(jax.random.fold_in(key_of[7], 71), 0)
    return dict(tokens=tokens, w_uvqk=w_uvqk, w_out=w_out, hist_len=hist_len, owner=owner, recv_offset=recv_offset, block_start=block_start)


EPS = 1e-05

def norm_rows(values):
    average = lax.optimization_barrier(jnp.mean(values, axis=-1, keepdims=True))
    variance = lax.optimization_barrier(jnp.mean(values * values, axis=-1, keepdims=True)) - average * average
    return (values - average) * lax.rsqrt(variance + EPS)

def rounded(values):
    return lax.optimization_barrier(values.astype(jnp.bfloat16)).astype(jnp.float32)

def reference(tokens, w_uvqk, w_out, hist_len, owner, recv_offset, block_start):
    head_size = D // HEADS
    window_rows = MAXB * BLOCK
    total_rows = tokens.shape[0]
    device_count = hist_len.shape[0]
    user_count = hist_len.shape[1]
    padded = jnp.concatenate([tokens, jnp.zeros((window_rows, D), tokens.dtype)], 0)
    position = jnp.arange(window_rows, dtype=jnp.int32)
    causal = position[None, :] <= position[:, None]
    device_ids = (jnp.arange(device_count * user_count, dtype=jnp.int32) // user_count).astype(jnp.int32)
    flat_len = hist_len.reshape(-1).astype(jnp.int32)
    flat_start = block_start.reshape(-1).astype(jnp.int32)
    flat_owner = owner.reshape(-1).astype(jnp.int32)
    flat_offset = recv_offset.reshape(-1).astype(jnp.int32)

    def one_user(user_item):
        device_id, length, start = user_item
        first_row = ((device_id * BLK_DEV + start) * BLOCK).astype(jnp.int32)
        rows_in = lax.dynamic_slice_in_dim(padded, first_row, window_rows, 0)
        widened = rows_in.astype(jnp.float32)
        normed = norm_rows(widened).astype(jnp.bfloat16)
        projected = jax.nn.silu(jnp.dot(normed, w_uvqk, preferred_element_type=jnp.float32))
        pieces = rounded(projected).reshape(window_rows, HEADS, 4, head_size)
        raw_scores = jnp.einsum('ihd,jhd->hij', pieces[:, :, 2], pieces[:, :, 3]) * head_size ** (-0.5)
        allowed = causal & (position[None, :] < length)
        weights = rounded(jnp.where(allowed[None], jax.nn.silu(raw_scores) / window_rows, 0.0))
        attended = jnp.einsum('hij,jhd->ihd', weights, pieces[:, :, 1]).reshape(window_rows, D)
        gated_rows = (norm_rows(attended) * pieces[:, :, 0].reshape(window_rows, D)).astype(jnp.bfloat16)
        mixed_rows = jnp.dot(gated_rows, w_out, preferred_element_type=jnp.float32) + widened
        return mixed_rows.astype(jnp.bfloat16)
    outputs = lax.map(one_user, (device_ids, flat_len, flat_start))
    targets = ((flat_owner * BLK_DEV + flat_offset) * BLOCK)[:, None] + position[None, :]
    targets = jnp.where(position[None, :] < flat_len[:, None], targets, total_rows).astype(jnp.int32)
    packed = jnp.zeros((total_rows + 1, D), jnp.bfloat16)
    packed = packed.at[targets.reshape(-1)].set(outputs.reshape(-1, D))[:total_rows]
    user_state = outputs[jnp.arange(device_count * user_count, dtype=jnp.int32), flat_len - 1]
    return (packed, user_state)
```

```python
import functools

import jax
import jax.numpy as jnp
from jax import lax
from jax.experimental import pallas as pl
from jax.experimental.pallas import tpu as pltpu
from jax.sharding import PartitionSpec as P

D = 512
HEADS = 4
HEAD = 128
BLOCK = 128
WINDOW = 256
USERS = 24
BLK_DEV = 48
N_DP = 64
N_MP = 4
OWN = USERS // N_MP
CHUNKS = 2
UC = OWN // CHUNKS
TILE = 16
GROUPS = WINDOW // TILE
EPS = 1e-05
MESH = pl.DeviceIdType.MESH
BF16 = jnp.bfloat16
F32 = jnp.float32


def shift_of(i):
    return 2 * (i % 2) + (i // 2) % 2


def gated_silu(v):
    half = v * 0.5
    return half + half * jnp.tanh(half)


def main_kernel(
    tokens, w_in, w_out, len_v, own_v, off_v, len_s, own_s, start_s,
    landed, meta, states,
    tok, wbuf, wo, normed, att, gates, tab, pin_v, pin_s, st_send, st_recv, *rest,
):
    outgoing = rest[:CHUNKS]
    middle = rest[CHUNKS : 2 * CHUNKS]
    packed = rest[2 * CHUNKS : 3 * CHUNKS]
    (loc_sem, w_send, w_recv, f_send, f_recv, t_send, t_recv, s_send, s_recv,
     p1_send, p1_recv, p1_loc, p2_send, p2_recv, p2_loc, pin_sem) = rest[3 * CHUNKS :]
    me = lax.axis_index("dp")
    mp = lax.axis_index("mp")
    core = me % 2
    partner = me + 1 - 2 * core
    right = (mp + 1) % N_MP
    left = (mp + 3) % N_MP
    across = (mp + 2) % N_MP

    load_tok = pltpu.make_async_copy(tokens, tok, loc_sem.at[0])
    load_w = pltpu.make_async_copy(w_in, wbuf.at[mp], loc_sem.at[1])
    load_wo = pltpu.make_async_copy(w_out, wo, loc_sem.at[2])
    load_w.start()
    load_tok.start()
    load_wo.start()

    barrier = pltpu.get_barrier_semaphore()

    @pl.loop(1, N_DP)
    def _(t):
        pl.semaphore_signal(barrier, inc=1, device_id=((me + t) % N_DP, mp), device_id_type=MESH)

    for other in (right, left, across):
        pl.semaphore_signal(barrier, inc=1, device_id=(me, other), device_id_type=MESH)

    tab[me] = jnp.zeros((4, 128), jnp.int32)
    tab[me, 0:1, 0:USERS] = len_v[...]
    tab[me, 1:2, 0:USERS] = own_v[...]
    tab[me, 2:3, 0:USERS] = off_v[...]
    st_send[...] = jnp.zeros_like(st_send)

    load_tok.wait()

    def user_rows(k):
        start = start_s[0, mp * OWN + k]
        follow = jnp.minimum(start + 1, BLK_DEV - 1)
        return jnp.concatenate([tok[start], tok[follow]], axis=0).astype(F32)

    @pl.loop(0, OWN)
    def _(k):
        x = user_rows(k)
        mean = jnp.mean(x, axis=-1, keepdims=True)
        var = jnp.mean(x * x, axis=-1, keepdims=True) - mean * mean
        normed[k] = ((x - mean) * lax.rsqrt(var + EPS)).astype(BF16)

    load_w.wait()
    load_wo.wait()
    pl.semaphore_wait(barrier, N_DP - 1 + N_MP - 1)

    half = pl.ds(pl.multiple_of(core * 256, 256), 256)
    other_half = pl.ds(pl.multiple_of((1 - core) * 256, 256), 256)

    def send_w(shard, target, k):
        return pltpu.make_async_remote_copy(
            src_ref=wbuf.at[shard, half], dst_ref=wbuf.at[shard, half],
            send_sem=w_send.at[k], recv_sem=w_recv.at[k],
            device_id=(me, target), device_id_type=MESH,
        )

    def forward_w(shard, k):
        return pltpu.make_async_remote_copy(
            src_ref=wbuf.at[shard, half], dst_ref=wbuf.at[shard, half],
            send_sem=f_send.at[k], recv_sem=f_recv.at[k],
            device_id=(partner, mp), device_id_type=MESH,
        )

    to_right = send_w(mp, right, 0)
    to_left = send_w(mp, left, 1)
    to_right.start()
    to_left.start()

    @pl.loop(1, N_DP)
    def _(t):
        pltpu.make_async_remote_copy(
            src_ref=tab.at[me], dst_ref=tab.at[me], send_sem=t_send, recv_sem=t_recv,
            device_id=((me + t) % N_DP, mp), device_id_type=MESH,
        ).start()

    row_id = lax.broadcasted_iota(jnp.int32, (BLOCK, BLOCK), 0)
    col_id = lax.broadcasted_iota(jnp.int32, (BLOCK, BLOCK), 1)
    causal = col_id <= row_id
    scaling = float(HEAD) ** -0.5
    nt = (((1,), (1,)), ((), ()))

    def head_of_user(shard, k):
        projected = gated_silu(
            jnp.dot(normed[k], wbuf[shard], preferred_element_type=F32)
        ).astype(BF16)
        gates[k, shard] = projected[:, 0:HEAD]
        v = projected[:, HEAD : 2 * HEAD]
        q = projected[:, 2 * HEAD : 3 * HEAD]
        key = projected[:, 3 * HEAD :]
        diag = jnp.concatenate(
            [
                lax.dot_general(q[:BLOCK], key[:BLOCK], nt, preferred_element_type=F32),
                lax.dot_general(q[BLOCK:], key[BLOCK:], nt, preferred_element_type=F32),
            ],
            axis=0,
        )
        back = lax.dot_general(q[BLOCK:], key[:BLOCK], nt, preferred_element_type=F32)
        both = jnp.concatenate([causal, causal], axis=0)
        w_diag = jnp.where(both, gated_silu(diag * scaling), 0.0).astype(BF16)
        w_back = gated_silu(back * scaling).astype(BF16)
        att[k, shard, 0:BLOCK] = jnp.dot(w_diag[:BLOCK], v[:BLOCK], preferred_element_type=F32)
        att[k, shard, BLOCK:] = jnp.dot(
            jnp.concatenate([w_back, w_diag[BLOCK:]], axis=1), v, preferred_element_type=F32
        )

    def heads(shard):
        @pl.loop(0, OWN)
        def _(k):
            head_of_user(shard, k)

    heads(mp)

    to_right.wait_recv()
    from_left = forward_w(left, 0)
    from_left.start()
    to_left.wait_recv()
    from_right = forward_w(right, 1)
    from_right.start()
    onward_shard = jnp.where(core == 0, left, right)
    onward_target = jnp.where(core == 0, right, left)
    onward = send_w(onward_shard, onward_target, 2)
    onward.start()
    from_left.wait_recv()
    heads(left)
    from_right.wait_recv()
    onward.wait_recv()
    from_across = forward_w(across, 2)
    from_across.start()
    heads(right)
    from_across.wait_recv()

    def finish(k, buf, j):
        a = [att[k, h] for h in range(HEADS)]
        total = sum(jnp.sum(p, axis=-1, keepdims=True) for p in a)
        squares = sum(jnp.sum(p * p, axis=-1, keepdims=True) for p in a)
        mean = total * (1.0 / D)
        var = squares * (1.0 / D) - mean * mean
        scale = lax.rsqrt(var + EPS * float(WINDOW * WINDOW))
        gated = jnp.concatenate(
            [((p - mean) * scale * gates[k, h].astype(F32)).astype(BF16) for h, p in enumerate(a)],
            axis=1,
        )
        mixed = jnp.dot(gated, wo[...], preferred_element_type=F32) + user_rows(k)
        mixed = mixed.astype(BF16)
        last = len_s[0, mp * OWN + k] - 1
        rows = lax.broadcasted_iota(jnp.int32, (WINDOW, HEAD), 0)
        for q in range(N_MP):
            part = mixed[:, q * HEAD : (q + 1) * HEAD]
            buf[q, :, j] = part.reshape(GROUPS, TILE, HEAD)
            state = jnp.sum(jnp.where(rows == last, part.astype(F32), 0.0), axis=0, keepdims=True)
            st_send[q, pl.ds(k, 1)] = state

    def slots(c, count):
        return middle[c].at[pl.ds(0, count)]

    def wait_slots(c, count, sem):
        pltpu.make_async_copy(slots(c, count), slots(c, count), sem).wait()

    for c in range(CHUNKS):
        @pl.loop(0, UC)
        def _(j):
            head_of_user(across, c * UC + j)
            finish(c * UC + j, outgoing[c], j)

        if c == CHUNKS - 1:
            for n, other in enumerate((right, left, across)):
                pltpu.make_async_remote_copy(
                    src_ref=st_send.at[other], dst_ref=st_recv.at[mp],
                    send_sem=s_send.at[n], recv_sem=s_recv.at[n],
                    device_id=(me, other), device_id_type=MESH,
                ).start()

        @pl.loop(1, N_DP)
        def _(t):
            i = (me + 27 * t) % N_DP
            pltpu.make_async_remote_copy(
                src_ref=outgoing[c].at[(mp + shift_of(i)) % N_MP, i // 4],
                dst_ref=middle[c].at[me],
                send_sem=p1_send.at[c], recv_sem=p1_recv.at[c],
                device_id=(i, mp), device_id_type=MESH,
            ).start()

        pltpu.make_async_copy(
            outgoing[c].at[(mp + shift_of(me)) % N_MP, me // 4], middle[c].at[me], p1_loc.at[c]
        ).start()

    pltpu.make_async_copy(tab.at[pl.ds(0, N_DP - 1)], tab.at[pl.ds(0, N_DP - 1)], t_recv).wait()
    lane = lax.broadcasted_iota(jnp.int32, (1, 128), 1)

    def scan_tables(d, carry):
        pin, lens, offs = carry
        rows = tab[d]
        owners = rows[1:2]
        first = jnp.broadcast_to(owners[:, 0:1], (1, 128))
        mine = owners == me
        return (
            jnp.where(first == lane, d, pin),
            jnp.where(mine, rows[0:1], lens),
            jnp.where(mine, rows[2:3], offs),
        )

    zero_row = jnp.zeros((1, 128), jnp.int32)
    pin, lens, offs = lax.fori_loop(0, N_DP, scan_tables, (zero_row, zero_row, zero_row))
    pin_v[...] = pin
    meta[...] = jnp.zeros((8, 128), jnp.int32)
    meta[0:1] = lens
    meta[1:2] = offs
    to_scalars = pltpu.make_async_copy(pin_v, pin_s, pin_sem)
    to_scalars.start()
    to_scalars.wait()

    beta = shift_of(me)
    column = (mp + beta) % N_MP

    for c in range(CHUNKS):
        wait_slots(c, N_DP - 1, p1_recv.at[c])
        pltpu.make_async_copy(
            outgoing[c].at[(mp + shift_of(me)) % N_MP, me // 4], middle[c].at[me], p1_loc.at[c]
        ).wait()
        firsts = [
            own_s[0, mp * OWN + c * UC + j] - own_s[0, 0] for j in range(UC)
        ]

        @pl.loop(0, N_DP, unroll=4)
        def _(o):
            for j in range(UC):
                d = pin_s[0, (o - firsts[j]) & (N_DP - 1)]
                packed[c][o, j] = middle[c][d, j]

        dst = landed.at[me, pl.ds(c * UC, UC)]

        @pl.loop(1, N_DP)
        def _(t):
            o = (me + 27 * t) % N_DP
            pltpu.make_async_remote_copy(
                src_ref=packed[c].at[o], dst_ref=dst,
                send_sem=p2_send.at[c], recv_sem=p2_recv.at[c],
                device_id=(o, column), device_id_type=MESH,
            ).start()

        @pl.when(beta != 0)
        def _():
            pltpu.make_async_remote_copy(
                src_ref=packed[c].at[me], dst_ref=dst,
                send_sem=p2_send.at[c], recv_sem=p2_recv.at[c],
                device_id=(me, column), device_id_type=MESH,
            ).start()

        @pl.when(beta == 0)
        def _():
            pltpu.make_async_copy(packed[c].at[me], dst, p2_loc.at[c]).start()

    for n, other in enumerate((left, right, across)):
        pltpu.make_async_remote_copy(
            src_ref=st_send.at[other], dst_ref=st_recv.at[other],
            send_sem=s_send.at[n], recv_sem=s_recv.at[n],
            device_id=(me, other), device_id_type=MESH,
        ).wait()
    states[...] = st_recv[...]
    states[mp] = st_send[mp]

    for copy in (to_right, to_left, onward, from_left, from_right, from_across):
        copy.wait_send()
    pltpu.make_async_copy(tab.at[pl.ds(0, N_DP - 1)], tab.at[pl.ds(0, N_DP - 1)], t_send).wait()
    for c in range(CHUNKS):
        wait_slots(c, N_DP - 1, p1_send.at[c])

    for c in range(CHUNKS):
        @pl.when(beta != 0)
        def _():
            wait_slots(c, N_DP, p2_recv.at[c])
            wait_slots(c, N_DP, p2_send.at[c])

        @pl.when(beta == 0)
        def _():
            wait_slots(c, N_DP - 1, p2_recv.at[c])
            wait_slots(c, N_DP - 1, p2_send.at[c])
            pltpu.make_async_copy(
                packed[c].at[me], landed.at[me, pl.ds(c * UC, UC)], p2_loc.at[c]
            ).wait()


def unpack_kernel(landed, meta, states, out, state_out):
    mp = lax.axis_index("mp")

    @pl.loop(0, BLK_DEV)
    def _(b):
        out[pl.ds(b * 8, 8)] = jnp.zeros((8, TILE, HEAD), BF16)

    row = lax.broadcasted_iota(jnp.int32, (TILE, HEAD), 0)

    @pl.loop(0, USERS)
    def _(u):
        count = meta[0, u]
        first = meta[1, u]
        j = u % OWN
        delta = (mp - u // OWN + N_MP) % N_MP
        low = delta // 2 + 2 * (delta % 2)
        for s in range(2):
            @pl.when(count > s * BLOCK)
            def _():
                for r in range(8):
                    g = s * 8 + r
                    value = landed[4 * g + low, j].astype(F32)
                    value = jnp.where(row + g * TILE < count, value, 0.0)
                    out[(first + s) * 8 + r] = value.astype(BF16)

    for m in range(N_MP):
        for k in range(OWN):
            state_out[pl.ds(m * OWN + k, 1)] = states[m, pl.ds(k, 1)].astype(BF16)


def per_device(tokens, w_uvqk, w_out, hist_len, owner, recv_offset, block_start):
    any_spec = pl.BlockSpec(memory_space=pl.ANY)
    vmem = pl.BlockSpec(memory_space=pltpu.VMEM)
    smem = pl.BlockSpec(memory_space=pltpu.SMEM)
    dma = pltpu.SemaphoreType.DMA
    landed, meta, states = pl.pallas_call(
        main_kernel,
        out_shape=(
            jax.ShapeDtypeStruct((N_DP, OWN, TILE, HEAD), BF16),
            jax.ShapeDtypeStruct((8, 128), jnp.int32),
            jax.ShapeDtypeStruct((N_MP, 8, HEAD), F32),
        ),
        in_specs=[any_spec] * 3 + [vmem] * 3 + [smem] * 3,
        out_specs=(any_spec, vmem, vmem),
        scratch_shapes=[
            pltpu.VMEM((BLK_DEV, BLOCK, D), BF16),
            pltpu.VMEM((N_MP, D, D), BF16),
            pltpu.VMEM((D, D), BF16),
            pltpu.VMEM((OWN, WINDOW, D), BF16),
            pltpu.VMEM((OWN, HEADS, WINDOW, HEAD), F32),
            pltpu.VMEM((OWN, HEADS, WINDOW, HEAD), BF16),
            pltpu.VMEM((N_DP, 4, 128), jnp.int32),
            pltpu.VMEM((1, 128), jnp.int32),
            pltpu.SMEM((1, 128), jnp.int32),
            pltpu.VMEM((N_MP, 8, HEAD), F32),
            pltpu.VMEM((N_MP, 8, HEAD), F32),
        ]
        + [pltpu.VMEM((N_MP, GROUPS, UC, TILE, HEAD), BF16)] * CHUNKS
        + [pltpu.VMEM((N_DP, UC, TILE, HEAD), BF16)] * (2 * CHUNKS)
        + [
            dma((3,)), dma((3,)), dma((3,)), dma((3,)), dma((3,)), dma, dma, dma((3,)), dma((3,)),
            dma((CHUNKS,)), dma((CHUNKS,)), dma((CHUNKS,)),
            dma((CHUNKS,)), dma((CHUNKS,)), dma((CHUNKS,)), dma,
        ],
        compiler_params=pltpu.CompilerParams(collective_id=0, has_side_effects=True),
        name="layer_and_repack",
    )(
        tokens.reshape(BLK_DEV, BLOCK, D), w_uvqk, w_out,
        hist_len, owner, recv_offset, hist_len, owner, block_start,
    )
    packed, state = pl.pallas_call(
        unpack_kernel,
        out_shape=(
            jax.ShapeDtypeStruct((BLK_DEV * 8, TILE, HEAD), BF16),
            jax.ShapeDtypeStruct((USERS, HEAD), BF16),
        ),
        in_specs=[vmem, smem, vmem],
        out_specs=(vmem, vmem),
        name="unpack",
    )(landed, meta, states)
    return packed.reshape(BLK_DEV * BLOCK, HEAD), state


def solution(mesh):
    in_specs = (
        P("dp", None),
        P(None, "mp"),
        P(),
        P("dp", None),
        P("dp", None),
        P("dp", None),
        P("dp", None),
    )
    out_specs = (P("dp", "mp"), P("dp", "mp"))
    return jax.shard_map(
        per_device, mesh=mesh, in_specs=in_specs, out_specs=out_specs, check_vma=False
    )
```

```python
import functools

import jax
import jax.numpy as jnp
from jax import lax
from jax.experimental import pallas as pl
from jax.experimental.pallas import tpu as pltpu
from jax.sharding import PartitionSpec as P

D = 512
HEADS = 4
HEAD = 128
BLOCK = 128
WINDOW = 256
USERS = 24
BLK_DEV = 48
N_DP = 64
N_MP = 4
OWN = USERS // N_MP
EARLY = 3
LATE = OWN - EARLY
TILE = 16
GROUPS = WINDOW // TILE
EPS = 1e-05
MESH = pl.DeviceIdType.MESH
BF16 = jnp.bfloat16
F32 = jnp.float32


def shift_of(i):
    return 2 * (i % 2) + (i // 2) % 2


def gated_silu(v):
    half = v * 0.5
    return half + half * jnp.tanh(half)


def main_kernel(
    tokens, w_in, w_out, len_v, own_v, off_v, len_s, own_s, start_s,
    landed, landed_early, meta, states,
    tok, wbuf, wo, normed, att, gates, x_early, mix_early, tab, build, pin_v, pin_s, st_send, st_recv,
    out_early, mid_early, pack_early, in_early, out_late, mid_late, pack_late,
    loc_sem, w_send, w_recv, f_send, f_recv, t_send, t_recv, s_send, s_recv,
    e1_send, e1_recv, e1_loc, e2_send, e2_recv, e2_loc, x_send, x_recv, x_loc,
    l1_send, l1_recv, l1_loc, l2_send, l2_recv, l2_loc, pin_sem,
):
    me = lax.axis_index("dp")
    mp = lax.axis_index("mp")
    core = me % 2
    partner = me + 1 - 2 * core
    right = (mp + 1) % N_MP
    left = (mp + 3) % N_MP
    across = (mp + 2) % N_MP

    load_tok = pltpu.make_async_copy(tokens, tok, loc_sem.at[0])
    load_w = pltpu.make_async_copy(w_in, wbuf.at[mp], loc_sem.at[1])
    load_wo = pltpu.make_async_copy(w_out, wo, loc_sem.at[2])
    load_w.start()
    load_tok.start()
    load_wo.start()

    barrier = pltpu.get_barrier_semaphore()

    @pl.loop(1, N_DP)
    def _(t):
        pl.semaphore_signal(barrier, inc=1, device_id=((me + t) % N_DP, mp), device_id_type=MESH)

    for other in (right, left, across):
        pl.semaphore_signal(barrier, inc=1, device_id=(me, other), device_id_type=MESH)

    build[...] = jnp.zeros_like(build)
    build[0:1, 0:USERS] = len_v[...]
    build[1:2, 0:USERS] = own_v[...]
    build[2:3, 0:USERS] = off_v[...]
    tab[me] = (
        build[0:1]
        + pltpu.roll(build[1:2], USERS, 1)
        + pltpu.roll(build[2:3], 2 * USERS, 1)
    )
    st_send[...] = jnp.zeros_like(st_send)

    load_tok.wait()

    def user_blocks(k):
        start = start_s[0, mp * OWN + k]
        return tok[start], tok[jnp.minimum(start + 1, BLK_DEV - 1)]

    def user_rows(k):
        return jnp.concatenate(user_blocks(k), axis=0).astype(F32)

    for k in range(EARLY):
        for s, block in enumerate(user_blocks(k)):
            for q in range(N_MP):
                part = block[:, q * HEAD : (q + 1) * HEAD]
                out_early[q, s * 8 : s * 8 + 8, k] = part.reshape(8, TILE, HEAD)

    def normalize(k, x):
        mean = jnp.mean(x, axis=-1, keepdims=True)
        var = jnp.mean(x * x, axis=-1, keepdims=True) - mean * mean
        normed[k] = ((x - mean) * lax.rsqrt(var + EPS)).astype(BF16)

    @pl.loop(0, OWN)
    def _(k):
        normalize(k, user_rows(k))

    load_w.wait()
    load_wo.wait()
    pl.semaphore_wait(barrier, N_DP - 1 + N_MP - 1)

    half = pl.ds(pl.multiple_of(core * 256, 256), 256)

    def send_w(shard, target, k):
        return pltpu.make_async_remote_copy(
            src_ref=wbuf.at[shard, half], dst_ref=wbuf.at[shard, half],
            send_sem=w_send.at[k], recv_sem=w_recv.at[k],
            device_id=(me, target), device_id_type=MESH,
        )

    def forward_w(shard, k):
        return pltpu.make_async_remote_copy(
            src_ref=wbuf.at[shard, half], dst_ref=wbuf.at[shard, half],
            send_sem=f_send.at[k], recv_sem=f_recv.at[k],
            device_id=(partner, mp), device_id_type=MESH,
        )

    to_right = send_w(mp, right, 0)
    to_left = send_w(mp, left, 1)
    to_right.start()
    to_left.start()

    @pl.loop(1, N_DP)
    def _(t):
        pltpu.make_async_remote_copy(
            src_ref=tab.at[me], dst_ref=tab.at[me], send_sem=t_send, recv_sem=t_recv,
            device_id=((me + t) % N_DP, mp), device_id_type=MESH,
        ).start()

    @pl.loop(1, N_DP)
    def _(t):
        i = (me + 27 * t) % N_DP
        pltpu.make_async_remote_copy(
            src_ref=out_early.at[i % 4, i // 4], dst_ref=mid_early.at[me],
            send_sem=e1_send, recv_sem=e1_recv,
            device_id=(i, mp), device_id_type=MESH,
        ).start()

    own_early = pltpu.make_async_copy(out_early.at[me % 4, me // 4], mid_early.at[me], e1_loc)
    own_early.start()

    row_id = lax.broadcasted_iota(jnp.int32, (BLOCK, BLOCK), 0)
    col_id = lax.broadcasted_iota(jnp.int32, (BLOCK, BLOCK), 1)
    causal = col_id <= row_id
    scaling = float(HEAD) ** -0.5
    nt = (((1,), (1,)), ((), ()))

    def head_of_user(shard, k):
        projected = gated_silu(
            jnp.dot(normed[k], wbuf[shard], preferred_element_type=F32)
        ).astype(BF16)
        gates[k, shard] = projected[:, 0:HEAD]
        v = projected[:, HEAD : 2 * HEAD]
        q = projected[:, 2 * HEAD : 3 * HEAD]
        key = projected[:, 3 * HEAD :]
        diag = jnp.concatenate(
            [
                lax.dot_general(q[:BLOCK], key[:BLOCK], nt, preferred_element_type=F32),
                lax.dot_general(q[BLOCK:], key[BLOCK:], nt, preferred_element_type=F32),
            ],
            axis=0,
        )
        back = lax.dot_general(q[BLOCK:], key[:BLOCK], nt, preferred_element_type=F32)
        both = jnp.concatenate([causal, causal], axis=0)
        w_diag = jnp.where(both, gated_silu(diag * scaling), 0.0).astype(BF16)
        w_back = gated_silu(back * scaling).astype(BF16)
        att[k, shard, 0:BLOCK] = jnp.dot(w_diag[:BLOCK], v[:BLOCK], preferred_element_type=F32)
        att[k, shard, BLOCK:] = jnp.dot(
            jnp.concatenate([w_back, w_diag[BLOCK:]], axis=1), v, preferred_element_type=F32
        )

    def heads(shard, low, high):
        @pl.loop(low, high)
        def _(k):
            head_of_user(shard, k)

    def finish(k, x):
        a = [att[k, h] for h in range(HEADS)]
        total = sum(jnp.sum(p, axis=-1, keepdims=True) for p in a)
        squares = sum(jnp.sum(p * p, axis=-1, keepdims=True) for p in a)
        mean = total * (1.0 / D)
        var = squares * (1.0 / D) - mean * mean
        scale = lax.rsqrt(var + EPS * float(WINDOW * WINDOW))
        gated = jnp.concatenate(
            [((p - mean) * scale * gates[k, h].astype(F32)).astype(BF16) for h, p in enumerate(a)],
            axis=1,
        )
        mixed = jnp.dot(gated, wo[...], preferred_element_type=F32) + x
        return mixed.astype(BF16)

    def keep_state(k, mixed):
        last = len_s[0, mp * OWN + k] - 1
        rows = lax.broadcasted_iota(jnp.int32, (WINDOW, HEAD), 0)
        for q in range(N_MP):
            part = mixed[:, q * HEAD : (q + 1) * HEAD].astype(F32)
            state = jnp.sum(jnp.where(rows == last, part, 0.0), axis=0, keepdims=True)
            st_send[q, pl.ds(k, 1)] = state

    heads(mp, EARLY, OWN)

    to_right.wait_recv()
    from_left = forward_w(left, 0)
    from_left.start()
    to_left.wait_recv()
    from_right = forward_w(right, 1)
    from_right.start()
    onward_shard = jnp.where(core == 0, left, right)
    onward_target = jnp.where(core == 0, right, left)
    onward = send_w(onward_shard, onward_target, 2)
    onward.start()
    from_left.wait_recv()
    heads(left, EARLY, OWN)
    from_right.wait_recv()
    heads(right, EARLY, OWN)
    onward.wait_recv()
    from_across = forward_w(across, 2)
    from_across.start()
    from_across.wait_recv()

    @pl.loop(0, LATE)
    def _(j):
        k = EARLY + j
        head_of_user(across, k)
        mixed = finish(k, user_rows(k))
        for q in range(N_MP):
            part = mixed[:, q * HEAD : (q + 1) * HEAD]
            out_late[q, :, j] = part.reshape(GROUPS, TILE, HEAD)
        keep_state(k, mixed)

    @pl.loop(1, N_DP)
    def _(t):
        i = (me + 27 * t) % N_DP
        pltpu.make_async_remote_copy(
            src_ref=out_late.at[(mp + shift_of(i)) % N_MP, i // 4], dst_ref=mid_late.at[me],
            send_sem=l1_send, recv_sem=l1_recv,
            device_id=(i, mp), device_id_type=MESH,
        ).start()

    own_late = pltpu.make_async_copy(
        out_late.at[(mp + shift_of(me)) % N_MP, me // 4], mid_late.at[me], l1_loc
    )
    own_late.start()

    def wait_slots(ref, count, sem):
        some = ref.at[pl.ds(0, count)]
        pltpu.make_async_copy(some, some, sem).wait()

    wait_slots(tab, N_DP - 1, t_recv)
    lane = lax.broadcasted_iota(jnp.int32, (1, 128), 1)

    def scan_tables(d, carry):
        pin, lens, offs = carry
        rows = tab[d]
        owners = pltpu.roll(rows, 128 - USERS, 1)
        first = jnp.broadcast_to(owners[:, 0:1], (1, 128))
        mine = owners == me
        return (
            jnp.where(first == lane, d, pin),
            jnp.where(mine, rows, lens),
            jnp.where(mine, pltpu.roll(rows, 128 - 2 * USERS, 1), offs),
        )

    zero_row = jnp.zeros((1, 128), jnp.int32)
    pin, lens, offs = lax.fori_loop(
        0, N_DP, scan_tables, (zero_row, zero_row, zero_row), unroll=4
    )
    pin_v[...] = pin
    meta[...] = jnp.zeros((8, 128), jnp.int32)
    meta[0:1] = lens
    meta[1:2] = offs
    to_scalars = pltpu.make_async_copy(pin_v, pin_s, pin_sem)
    to_scalars.start()
    to_scalars.wait()

    def regroup(packed, middle, low, count):
        firsts = [own_s[0, mp * OWN + low + j] - own_s[0, 0] for j in range(count)]

        @pl.loop(0, N_DP, unroll=4)
        def _(o):
            for j in range(count):
                packed[o, j] = middle[pin_s[0, (o - firsts[j]) & (N_DP - 1)], j]

    wait_slots(mid_early, N_DP - 1, e1_recv)
    own_early.wait()
    regroup(pack_early, mid_early, 0, EARLY)

    @pl.loop(1, N_DP)
    def _(t):
        o = (me + 27 * t) % N_DP
        pltpu.make_async_remote_copy(
            src_ref=pack_early.at[o], dst_ref=in_early.at[me],
            send_sem=e2_send, recv_sem=e2_recv,
            device_id=(o, mp), device_id_type=MESH,
        ).start()

    kept_early = pltpu.make_async_copy(pack_early.at[me], in_early.at[me], e2_loc)
    kept_early.start()

    for shard in (mp, left, right):
        heads(shard, 0, EARLY)

    @pl.loop(0, EARLY)
    def _(k):
        head_of_user(across, k)
        keep_state(k, finish(k, user_rows(k)))

    state_copies = []
    for n, (other, source) in enumerate(((right, left), (left, right), (across, across))):
        copy = pltpu.make_async_remote_copy(
            src_ref=st_send.at[other], dst_ref=st_recv.at[mp],
            send_sem=s_send.at[n], recv_sem=s_recv.at[n],
            device_id=(me, other), device_id_type=MESH,
        )
        copy.start()
        state_copies.append(copy)

    beta = shift_of(me)
    column = (mp + beta) % N_MP
    wait_slots(mid_late, N_DP - 1, l1_recv)
    own_late.wait()
    regroup(pack_late, mid_late, EARLY, LATE)

    @pl.loop(1, N_DP)
    def _(t):
        o = (me + 27 * t) % N_DP
        pltpu.make_async_remote_copy(
            src_ref=pack_late.at[o], dst_ref=landed.at[me],
            send_sem=l2_send, recv_sem=l2_recv,
            device_id=(o, column), device_id_type=MESH,
        ).start()

    @pl.when(beta != 0)
    def _():
        pltpu.make_async_remote_copy(
            src_ref=pack_late.at[me], dst_ref=landed.at[me],
            send_sem=l2_send, recv_sem=l2_recv,
            device_id=(me, column), device_id_type=MESH,
        ).start()

    @pl.when(beta == 0)
    def _():
        pltpu.make_async_copy(pack_late.at[me], landed.at[me], l2_loc).start()

    wait_slots(in_early, N_DP - 1, e2_recv)
    kept_early.wait()

    @pl.loop(0, GROUPS)
    def _(g):
        rows = pl.ds(pl.multiple_of(g * TILE, TILE), TILE)
        for q in range(N_MP):
            for k in range(EARLY):
                x_early[k, rows, q * HEAD : (q + 1) * HEAD] = in_early[4 * g + q, k]

    for k in range(EARLY):
        normalize(k, x_early[k].astype(F32))

    for shard in (mp, left, right):
        heads(shard, 0, EARLY)

    for k in range(EARLY):
        head_of_user(across, k)
        mixed = finish(k, x_early[k].astype(F32))
        for q in range(N_MP):
            mix_early[q, k] = mixed[:, q * HEAD : (q + 1) * HEAD]
        for n, other in enumerate((right, left, across)):
            pltpu.make_async_remote_copy(
                src_ref=mix_early.at[other, k], dst_ref=landed_early.at[mp, k],
                send_sem=x_send.at[n], recv_sem=x_recv.at[n],
                device_id=(me, other), device_id_type=MESH,
            ).start()

    kept = pltpu.make_async_copy(mix_early.at[mp], landed_early.at[mp], x_loc)
    kept.start()

    for copy in state_copies:
        copy.wait()
    for m in range(N_MP):
        @pl.when(m != mp)
        def _():
            states[m] = st_recv[m]

        @pl.when(m == mp)
        def _():
            states[m] = st_send[m]

    for copy in (to_right, to_left, onward, from_left, from_right, from_across):
        copy.wait_send()
    wait_slots(tab, N_DP - 1, t_send)
    wait_slots(mid_early, N_DP - 1, e1_send)
    wait_slots(mid_early, N_DP - 1, e2_send)
    wait_slots(mid_late, N_DP - 1, l1_send)
    for n, (other, source) in enumerate(((right, left), (left, right), (across, across))):
        pltpu.make_async_remote_copy(
            src_ref=mix_early.at[other], dst_ref=landed_early.at[source],
            send_sem=x_send.at[n], recv_sem=x_recv.at[n],
            device_id=(me, other), device_id_type=MESH,
        ).wait()
    kept.wait()

    @pl.when(beta != 0)
    def _():
        wait_slots(mid_late, N_DP, l2_recv)
        wait_slots(mid_late, N_DP, l2_send)

    @pl.when(beta == 0)
    def _():
        wait_slots(mid_late, N_DP - 1, l2_recv)
        wait_slots(mid_late, N_DP - 1, l2_send)
        pltpu.make_async_copy(pack_late.at[me], landed.at[me], l2_loc).wait()


def unpack_kernel(landed, landed_early, meta, states, out, state_out):
    mp = lax.axis_index("mp")

    @pl.loop(0, BLK_DEV)
    def _(b):
        out[pl.ds(b * 8, 8)] = jnp.zeros((8, TILE, HEAD), BF16)

    row = lax.broadcasted_iota(jnp.int32, (TILE, HEAD), 0)

    def place(u, g, value):
        count = meta[0, u]
        value = jnp.where(row + g * TILE < count, value.astype(F32), 0.0)
        out[meta[1, u] * 8 + g] = value.astype(BF16)

    for m in range(N_MP):
        delta = (mp - m + N_MP) % N_MP
        low = delta // 2 + 2 * (delta % 2)

        @pl.loop(0, OWN)
        def _(k):
            u = m * OWN + k
            for s in range(2):
                @pl.when((meta[0, u] > s * BLOCK) & (k < EARLY))
                def _():
                    for r in range(8):
                        g = s * 8 + r
                        place(u, g, landed_early[m, k, g])

                @pl.when((meta[0, u] > s * BLOCK) & (k >= EARLY))
                def _():
                    for r in range(8):
                        g = s * 8 + r
                        place(u, g, landed[4 * g + low, k - EARLY])

    for m in range(N_MP):
        for k in range(OWN):
            state_out[pl.ds(m * OWN + k, 1)] = states[m, pl.ds(k, 1)].astype(BF16)


def per_device(tokens, w_uvqk, w_out, hist_len, owner, recv_offset, block_start):
    any_spec = pl.BlockSpec(memory_space=pl.ANY)
    vmem = pl.BlockSpec(memory_space=pltpu.VMEM)
    smem = pl.BlockSpec(memory_space=pltpu.SMEM)
    dma = pltpu.SemaphoreType.DMA
    landed, landed_early, meta, states = pl.pallas_call(
        main_kernel,
        out_shape=(
            jax.ShapeDtypeStruct((N_DP, LATE, TILE, HEAD), BF16),
            jax.ShapeDtypeStruct((N_MP, EARLY, WINDOW, HEAD), BF16),
            jax.ShapeDtypeStruct((8, 128), jnp.int32),
            jax.ShapeDtypeStruct((N_MP, 8, HEAD), F32),
        ),
        in_specs=[any_spec] * 3 + [vmem] * 3 + [smem] * 3,
        out_specs=(any_spec, any_spec, vmem, vmem),
        scratch_shapes=[
            pltpu.VMEM((BLK_DEV, BLOCK, D), BF16),
            pltpu.VMEM((N_MP, D, D), BF16),
            pltpu.VMEM((D, D), BF16),
            pltpu.VMEM((OWN, WINDOW, D), BF16),
            pltpu.VMEM((OWN, HEADS, WINDOW, HEAD), F32),
            pltpu.VMEM((OWN, HEADS, WINDOW, HEAD), BF16),
            pltpu.VMEM((EARLY, WINDOW, D), BF16),
            pltpu.VMEM((N_MP, EARLY, WINDOW, HEAD), BF16),
            pltpu.VMEM((N_DP, 1, 128), jnp.int32),
            pltpu.VMEM((8, 128), jnp.int32),
            pltpu.VMEM((1, 128), jnp.int32),
            pltpu.SMEM((1, 128), jnp.int32),
            pltpu.VMEM((N_MP, 8, HEAD), F32),
            pltpu.VMEM((N_MP, 8, HEAD), F32),
            pltpu.VMEM((N_MP, GROUPS, EARLY, TILE, HEAD), BF16),
            pltpu.VMEM((N_DP, EARLY, TILE, HEAD), BF16),
            pltpu.VMEM((N_DP, EARLY, TILE, HEAD), BF16),
            pltpu.VMEM((N_DP, EARLY, TILE, HEAD), BF16),
            pltpu.VMEM((N_MP, GROUPS, LATE, TILE, HEAD), BF16),
            pltpu.VMEM((N_DP, LATE, TILE, HEAD), BF16),
            pltpu.VMEM((N_DP, LATE, TILE, HEAD), BF16),
            dma((3,)), dma((3,)), dma((3,)), dma((3,)), dma((3,)), dma, dma, dma((3,)), dma((3,)),
            dma, dma, dma, dma, dma, dma, dma((3,)), dma((3,)), dma,
            dma, dma, dma, dma, dma, dma, dma,
        ],
        compiler_params=pltpu.CompilerParams(collective_id=0, has_side_effects=True),
        name="layer_and_repack",
    )(
        tokens.reshape(BLK_DEV, BLOCK, D), w_uvqk, w_out,
        hist_len, owner, recv_offset, hist_len, owner, block_start,
    )
    packed, state = pl.pallas_call(
        unpack_kernel,
        out_shape=(
            jax.ShapeDtypeStruct((BLK_DEV * 8, TILE, HEAD), BF16),
            jax.ShapeDtypeStruct((USERS, HEAD), BF16),
        ),
        in_specs=[vmem, vmem, smem, vmem],
        out_specs=(vmem, vmem),
        name="unpack",
    )(landed, landed_early.reshape(N_MP, EARLY, GROUPS, TILE, HEAD), meta, states)
    return packed.reshape(BLK_DEV * BLOCK, HEAD), state


def solution(mesh):
    in_specs = (
        P("dp", None),
        P(None, "mp"),
        P(),
        P("dp", None),
        P("dp", None),
        P("dp", None),
        P("dp", None),
    )
    out_specs = (P("dp", "mp"), P("dp", "mp"))
    return jax.shard_map(
        per_device, mesh=mesh, in_specs=in_specs, out_specs=out_specs, check_vma=False
    )
```

```python
import functools

import jax
import jax.numpy as jnp
from jax import lax
from jax.experimental import pallas as pl
from jax.experimental.pallas import tpu as pltpu
from jax.sharding import PartitionSpec as P

D = 512
HEADS = 4
HEAD = 128
BLOCK = 128
WINDOW = 256
USERS = 24
BLK_DEV = 48
N_DP = 64
N_MP = 4
OWN = USERS // N_MP
PARTS = (2, 1)
EARLY = sum(PARTS)
CHUNKS = len(PARTS)
STARTS = tuple(sum(PARTS[:c]) for c in range(CHUNKS))
LATE = OWN - EARLY
TILE = 16
GROUPS = WINDOW // TILE
EPS = 1e-05
MESH = pl.DeviceIdType.MESH
BF16 = jnp.bfloat16
F32 = jnp.float32


def shift_of(i):
    return 2 * (i % 2) + (i // 2) % 2


def gated_silu(v):
    half = v * 0.5
    return half + half * jnp.tanh(half)


def main_kernel(
    tokens, w_in, w_out, len_in, own_in, off_in, start_in,
    landed, landed_early, meta, states,
    tok, wbuf, wo, normed, att, gates, x_early, mix_early, tab, build, pin_v, pin_s, st_send, st_recv,
    len_v, own_v, off_v, len_s, own_s, start_s, out_late, mid_late, pack_late, *rest,
):
    out_early, mid_early, pack_early, in_early = (
        rest[n * CHUNKS : (n + 1) * CHUNKS] for n in range(4)
    )
    (loc_sem, in_sem, w_send, w_recv, f_send, f_recv, t_send, t_recv, s_send, s_recv,
    e1_send, e1_recv, e1_loc, e2_send, e2_recv, e2_loc, x_send, x_recv, x_loc,
    l1_send, l1_recv, l1_loc, l2_send, l2_recv, l2_loc, pin_sem) = rest[4 * CHUNKS :]
    me = lax.axis_index("dp")
    mp = lax.axis_index("mp")
    core = me % 2
    partner = me + 1 - 2 * core
    right = (mp + 1) % N_MP
    left = (mp + 3) % N_MP
    across = (mp + 2) % N_MP

    load_tok = pltpu.make_async_copy(tokens, tok, loc_sem.at[0])
    load_tok.start()
    small = [
        pltpu.make_async_copy(src, dst, in_sem.at[n])
        for n, (src, dst) in enumerate(
            (
                (start_in, start_s), (len_in, len_v), (own_in, own_v), (off_in, off_v),
                (len_in, len_s), (own_in, own_s),
            )
        )
    ]
    load_w = pltpu.make_async_copy(w_in, wbuf.at[mp], loc_sem.at[1])
    load_wo = pltpu.make_async_copy(w_out, wo, loc_sem.at[2])
    for copy in small:
        copy.start()
    load_w.start()
    load_wo.start()

    barrier = pltpu.get_barrier_semaphore()

    def greet(peer):
        pl.semaphore_signal(barrier, inc=1, device_id=(peer % N_DP, mp), device_id_type=MESH)

    greet(me + N_DP // 2)

    @pl.loop(1, N_DP // 2)
    def _(t):
        greet(me + N_DP // 2 + t)
        greet(me + N_DP // 2 - t)

    for other in (right, left, across):
        pl.semaphore_signal(barrier, inc=1, device_id=(me, other), device_id_type=MESH)

    for copy in small:
        copy.wait()

    build[...] = jnp.zeros_like(build)
    build[0:1, 0:USERS] = len_v[...]
    build[1:2, 0:USERS] = own_v[...]
    build[2:3, 0:USERS] = off_v[...]
    tab[me] = (
        build[0:1]
        + pltpu.roll(build[1:2], USERS, 1)
        + pltpu.roll(build[2:3], 2 * USERS, 1)
    )
    st_send[...] = jnp.zeros_like(st_send)

    load_tok.wait()

    def user_blocks(k):
        start = start_s[0, mp * OWN + k]
        return tok[start], tok[jnp.minimum(start + 1, BLK_DEV - 1)]

    def user_rows(k):
        return jnp.concatenate(user_blocks(k), axis=0).astype(F32)

    for k in range(EARLY):
        for s, block in enumerate(user_blocks(k)):
            for q in range(N_MP):
                part = block[:, q * HEAD : (q + 1) * HEAD]
                c = sum(k >= low for low in STARTS) - 1
                out_early[c][q, s * 8 : s * 8 + 8, k - STARTS[c]] = part.reshape(8, TILE, HEAD)

    load_w.wait()
    pl.semaphore_wait(barrier, N_DP - 1 + N_MP - 1)

    half = pl.ds(pl.multiple_of(core * 256, 256), 256)

    def send_w(shard, target, k):
        return pltpu.make_async_remote_copy(
            src_ref=wbuf.at[shard, half], dst_ref=wbuf.at[shard, half],
            send_sem=w_send.at[k], recv_sem=w_recv.at[k],
            device_id=(me, target), device_id_type=MESH,
        )

    def forward_w(shard, k):
        return pltpu.make_async_remote_copy(
            src_ref=wbuf.at[shard, half], dst_ref=wbuf.at[shard, half],
            send_sem=f_send.at[k], recv_sem=f_recv.at[k],
            device_id=(partner, mp), device_id_type=MESH,
        )

    to_right = send_w(mp, right, 0)
    to_left = send_w(mp, left, 1)
    to_right.start()
    to_left.start()

    def send_tables():
        @pl.loop(1, N_DP)
        def _(t):
            pltpu.make_async_remote_copy(
                src_ref=tab.at[me], dst_ref=tab.at[me], send_sem=t_send, recv_sem=t_recv,
                device_id=((me + t) % N_DP, mp), device_id_type=MESH,
            ).start()

    own_early = []
    for c in range(CHUNKS):
        @pl.loop(1, N_DP)
        def _(t):
            i = (me + 27 * t) % N_DP
            pltpu.make_async_remote_copy(
                src_ref=out_early[c].at[i % 4, i // 4], dst_ref=mid_early[c].at[me],
                send_sem=e1_send.at[c], recv_sem=e1_recv.at[c],
                device_id=(i, mp), device_id_type=MESH,
            ).start()

        copy = pltpu.make_async_copy(
            out_early[c].at[me % 4, me // 4], mid_early[c].at[me], e1_loc.at[c]
        )
        copy.start()
        own_early.append(copy)
        if c == 0:
            send_tables()

    load_wo.wait()
    def normalize(k, x):
        mean = jnp.mean(x, axis=-1, keepdims=True)
        var = jnp.mean(x * x, axis=-1, keepdims=True) - mean * mean
        normed[k] = ((x - mean) * lax.rsqrt(var + EPS)).astype(BF16)

    @pl.loop(EARLY, OWN)
    def _(k):
        normalize(k, user_rows(k))

    row_id = lax.broadcasted_iota(jnp.int32, (BLOCK, BLOCK), 0)
    col_id = lax.broadcasted_iota(jnp.int32, (BLOCK, BLOCK), 1)
    causal = col_id <= row_id
    scaling = float(HEAD) ** -0.5
    nt = (((1,), (1,)), ((), ()))

    def head_of_user(shard, k):
        projected = gated_silu(
            jnp.dot(normed[k], wbuf[shard], preferred_element_type=F32)
        ).astype(BF16)
        gates[k, shard] = projected[:, 0:HEAD]
        v = projected[:, HEAD : 2 * HEAD]
        q = projected[:, 2 * HEAD : 3 * HEAD]
        key = projected[:, 3 * HEAD :]
        diag = jnp.concatenate(
            [
                lax.dot_general(q[:BLOCK], key[:BLOCK], nt, preferred_element_type=F32),
                lax.dot_general(q[BLOCK:], key[BLOCK:], nt, preferred_element_type=F32),
            ],
            axis=0,
        )
        back = lax.dot_general(q[BLOCK:], key[:BLOCK], nt, preferred_element_type=F32)
        both = jnp.concatenate([causal, causal], axis=0)
        w_diag = jnp.where(both, gated_silu(diag * scaling), 0.0).astype(BF16)
        w_back = gated_silu(back * scaling).astype(BF16)
        att[k, shard, 0:BLOCK] = jnp.dot(w_diag[:BLOCK], v[:BLOCK], preferred_element_type=F32)
        att[k, shard, BLOCK:] = jnp.dot(
            jnp.concatenate([w_back, w_diag[BLOCK:]], axis=1), v, preferred_element_type=F32
        )

    def heads(shard, low, high):
        @pl.loop(low, high)
        def _(k):
            head_of_user(shard, k)

    heads(mp, EARLY, OWN)

    def finish(k, x):
        a = [att[k, h] for h in range(HEADS)]
        total = sum(jnp.sum(p, axis=-1, keepdims=True) for p in a)
        squares = sum(jnp.sum(p * p, axis=-1, keepdims=True) for p in a)
        mean = total * (1.0 / D)
        var = squares * (1.0 / D) - mean * mean
        scale = lax.rsqrt(var + EPS * float(WINDOW * WINDOW))
        gated = jnp.concatenate(
            [((p - mean) * scale * gates[k, h].astype(F32)).astype(BF16) for h, p in enumerate(a)],
            axis=1,
        )
        mixed = jnp.dot(gated, wo[...], preferred_element_type=F32) + x
        return mixed.astype(BF16)

    def keep_state(k, mixed):
        last = len_s[0, mp * OWN + k] - 1
        rows = lax.broadcasted_iota(jnp.int32, (WINDOW, HEAD), 0)
        for q in range(N_MP):
            part = mixed[:, q * HEAD : (q + 1) * HEAD].astype(F32)
            state = jnp.sum(jnp.where(rows == last, part, 0.0), axis=0, keepdims=True)
            st_send[q, pl.ds(k, 1)] = state

    to_right.wait_recv()
    from_left = forward_w(left, 0)
    from_left.start()
    to_left.wait_recv()
    from_right = forward_w(right, 1)
    from_right.start()
    onward_shard = jnp.where(core == 0, left, right)
    onward_target = jnp.where(core == 0, right, left)
    onward = send_w(onward_shard, onward_target, 2)
    onward.start()
    from_left.wait_recv()
    heads(left, EARLY, OWN)
    from_right.wait_recv()
    heads(right, EARLY, OWN)
    onward.wait_recv()
    from_across = forward_w(across, 2)
    from_across.start()
    from_across.wait_recv()

    @pl.loop(0, LATE)
    def _(j):
        k = EARLY + j
        head_of_user(across, k)
        mixed = finish(k, user_rows(k))
        for q in range(N_MP):
            part = mixed[:, q * HEAD : (q + 1) * HEAD]
            out_late[q, :, j] = part.reshape(GROUPS, TILE, HEAD)
        keep_state(k, mixed)

    def send_late(i, hop):
        column = (mp + hop) % N_MP
        pltpu.make_async_remote_copy(
            src_ref=out_late.at[column, i // 4], dst_ref=mid_late.at[me],
            send_sem=l1_send, recv_sem=l1_recv,
            device_id=(i, column), device_id_type=MESH,
        ).start()

    @pl.loop(1, N_DP)
    def _(t):
        i = (me + 27 * t) % N_DP
        send_late(i, shift_of(i))

    hop = shift_of(me)

    @pl.when(hop != 0)
    def _():
        send_late(me, hop)

    @pl.when(hop == 0)
    def _():
        pltpu.make_async_copy(out_late.at[mp, me // 4], mid_late.at[me], l1_loc).start()

    def wait_slots(ref, count, sem):
        some = ref.at[pl.ds(0, count)]
        pltpu.make_async_copy(some, some, sem).wait()

    wait_slots(tab, N_DP - 1, t_recv)
    rows = tab[...].reshape(N_DP, 128)
    owners = pltpu.roll(rows, 128 - USERS, 1)
    offsets = pltpu.roll(rows, 128 - 2 * USERS, 1)
    lane = lax.broadcasted_iota(jnp.int32, (N_DP, 128), 1)
    source = lax.broadcasted_iota(jnp.int32, (N_DP, 128), 0)

    def pick(mask, values):
        return jnp.max(jnp.where(mask, values, 0), axis=0, keepdims=True)

    pin = pick(owners[:, 0:1] == lane, source)
    lens = pick(owners == me, rows)
    offs = pick(owners == me, offsets)
    pin_v[...] = pin
    meta[...] = jnp.zeros((8, 128), jnp.int32)
    meta[0:1] = lens
    meta[1:2] = offs
    to_scalars = pltpu.make_async_copy(pin_v, pin_s, pin_sem)
    to_scalars.start()
    to_scalars.wait()

    def regroup(packed, middle, low, count):
        firsts = [own_s[0, low + j] - own_s[0, 0] for j in range(count)]

        @pl.loop(0, N_DP, unroll=4)
        def _(o):
            for j in range(count):
                packed[o, j] = middle[pin_s[0, (o - firsts[j]) & (N_DP - 1)], j]

    kept_early = []
    for c in range(CHUNKS):
        wait_slots(mid_early[c], N_DP - 1, e1_recv.at[c])
        own_early[c].wait()
        regroup(pack_early[c], mid_early[c], mp * OWN + STARTS[c], PARTS[c])

        @pl.loop(1, N_DP)
        def _(t):
            o = (me + 27 * t) % N_DP
            pltpu.make_async_remote_copy(
                src_ref=pack_early[c].at[o], dst_ref=in_early[c].at[me],
                send_sem=e2_send.at[c], recv_sem=e2_recv.at[c],
                device_id=(o, mp), device_id_type=MESH,
            ).start()

        copy = pltpu.make_async_copy(pack_early[c].at[me], in_early[c].at[me], e2_loc.at[c])
        copy.start()
        kept_early.append(copy)

    @pl.loop(0, EARLY)
    def _(k):
        normalize(k, user_rows(k))

    for shard in (mp, left, right):
        heads(shard, 0, EARLY)

    @pl.loop(0, EARLY)
    def _(k):
        head_of_user(across, k)
        keep_state(k, finish(k, user_rows(k)))

    state_copies = []
    for n, (other, source) in enumerate(((right, left), (left, right), (across, across))):
        copy = pltpu.make_async_remote_copy(
            src_ref=st_send.at[other], dst_ref=st_recv.at[mp],
            send_sem=s_send.at[n], recv_sem=s_recv.at[n],
            device_id=(me, other), device_id_type=MESH,
        )
        copy.start()
        state_copies.append(copy)

    @pl.when(hop != 0)
    def _():
        wait_slots(mid_late, N_DP, l1_recv)

    @pl.when(hop == 0)
    def _():
        wait_slots(mid_late, N_DP - 1, l1_recv)
        pltpu.make_async_copy(out_late.at[mp, me // 4], mid_late.at[me], l1_loc).wait()

    regroup(pack_late, mid_late, (mp - hop + N_MP) % N_MP * OWN + EARLY, LATE)

    @pl.loop(1, N_DP)
    def _(t):
        o = (me + 27 * t) % N_DP
        pltpu.make_async_remote_copy(
            src_ref=pack_late.at[o], dst_ref=landed.at[me],
            send_sem=l2_send, recv_sem=l2_recv,
            device_id=(o, mp), device_id_type=MESH,
        ).start()

    kept_late = pltpu.make_async_copy(pack_late.at[me], landed.at[me], l2_loc)
    kept_late.start()

    for c in range(CHUNKS):
        wait_slots(in_early[c], N_DP - 1, e2_recv.at[c])
        kept_early[c].wait()
        mine = range(STARTS[c], STARTS[c] + PARTS[c])

        @pl.loop(0, GROUPS)
        def _(g):
            rows = pl.ds(pl.multiple_of(g * TILE, TILE), TILE)
            for q in range(N_MP):
                for k in mine:
                    x_early[k, rows, q * HEAD : (q + 1) * HEAD] = in_early[c][4 * g + q, k - STARTS[c]]

        for k in mine:
            normalize(k, x_early[k].astype(F32))

        for shard in (mp, left, right):
            heads(shard, mine[0], mine[0] + PARTS[c])

        @pl.loop(mine[0], mine[0] + PARTS[c])
        def _(k):
            head_of_user(across, k)
            mixed = finish(k, x_early[k].astype(F32))
            for q in range(N_MP):
                mix_early[q, k] = mixed[:, q * HEAD : (q + 1) * HEAD]
            for n, other in enumerate((right, left, across)):
                pltpu.make_async_remote_copy(
                    src_ref=mix_early.at[other, k], dst_ref=landed_early.at[mp, k],
                    send_sem=x_send.at[n], recv_sem=x_recv.at[n],
                    device_id=(me, other), device_id_type=MESH,
                ).start()

    kept = pltpu.make_async_copy(mix_early.at[mp], landed_early.at[mp], x_loc)
    kept.start()

    for copy in state_copies:
        copy.wait()
    for m in range(N_MP):
        @pl.when(m != mp)
        def _():
            states[m] = st_recv[m]

        @pl.when(m == mp)
        def _():
            states[m] = st_send[m]

    for copy in (to_right, to_left, onward, from_left, from_right, from_across):
        copy.wait_send()
    wait_slots(tab, N_DP - 1, t_send)
    for c in range(CHUNKS):
        wait_slots(mid_early[c], N_DP - 1, e1_send.at[c])
        wait_slots(mid_early[c], N_DP - 1, e2_send.at[c])

    @pl.when(hop != 0)
    def _():
        wait_slots(mid_late, N_DP, l1_send)

    @pl.when(hop == 0)
    def _():
        wait_slots(mid_late, N_DP - 1, l1_send)

    wait_slots(mid_late, N_DP - 1, l2_send)
    for n, (other, source) in enumerate(((right, left), (left, right), (across, across))):
        pltpu.make_async_remote_copy(
            src_ref=mix_early.at[other], dst_ref=landed_early.at[source],
            send_sem=x_send.at[n], recv_sem=x_recv.at[n],
            device_id=(me, other), device_id_type=MESH,
        ).wait()
    kept.wait()

    wait_slots(mid_late, N_DP - 1, l2_recv)
    kept_late.wait()


def unpack_kernel(landed, landed_early, meta, states, out, state_out):
    mp = lax.axis_index("mp")

    @pl.loop(0, BLK_DEV)
    def _(b):
        out[pl.ds(b * 8, 8)] = jnp.zeros((8, TILE, HEAD), BF16)

    row = lax.broadcasted_iota(jnp.int32, (TILE, HEAD), 0)

    def place(u, g, value):
        count = meta[0, u]
        value = jnp.where(row + g * TILE < count, value.astype(F32), 0.0)
        out[meta[1, u] * 8 + g] = value.astype(BF16)

    for m in range(N_MP):
        delta = (mp - m + N_MP) % N_MP
        low = delta // 2 + 2 * (delta % 2)

        @pl.loop(0, OWN)
        def _(k):
            u = m * OWN + k
            for s in range(2):
                @pl.when((meta[0, u] > s * BLOCK) & (k < EARLY))
                def _():
                    for r in range(8):
                        g = s * 8 + r
                        place(u, g, landed_early[m, k, g])

                @pl.when((meta[0, u] > s * BLOCK) & (k >= EARLY))
                def _():
                    for r in range(8):
                        g = s * 8 + r
                        place(u, g, landed[4 * g + low, k - EARLY])

    for m in range(N_MP):
        for k in range(OWN):
            state_out[pl.ds(m * OWN + k, 1)] = states[m, pl.ds(k, 1)].astype(BF16)


def per_device(tokens, w_uvqk, w_out, hist_len, owner, recv_offset, block_start):
    any_spec = pl.BlockSpec(memory_space=pl.ANY)
    vmem = pl.BlockSpec(memory_space=pltpu.VMEM)
    smem = pl.BlockSpec(memory_space=pltpu.SMEM)
    dma = pltpu.SemaphoreType.DMA
    landed, landed_early, meta, states = pl.pallas_call(
        main_kernel,
        out_shape=(
            jax.ShapeDtypeStruct((N_DP, LATE, TILE, HEAD), BF16),
            jax.ShapeDtypeStruct((N_MP, EARLY, WINDOW, HEAD), BF16),
            jax.ShapeDtypeStruct((8, 128), jnp.int32),
            jax.ShapeDtypeStruct((N_MP, 8, HEAD), F32),
        ),
        in_specs=[any_spec] * 7,
        out_specs=(vmem, vmem, vmem, vmem),
        scratch_shapes=[
            pltpu.VMEM((BLK_DEV, BLOCK, D), BF16),
            pltpu.VMEM((N_MP, D, D), BF16),
            pltpu.VMEM((D, D), BF16),
            pltpu.VMEM((OWN, WINDOW, D), BF16),
            pltpu.VMEM((OWN, HEADS, WINDOW, HEAD), F32),
            pltpu.VMEM((OWN, HEADS, WINDOW, HEAD), BF16),
            pltpu.VMEM((EARLY, WINDOW, D), BF16),
            pltpu.VMEM((N_MP, EARLY, WINDOW, HEAD), BF16),
            pltpu.VMEM((N_DP, 1, 128), jnp.int32),
            pltpu.VMEM((8, 128), jnp.int32),
            pltpu.VMEM((1, 128), jnp.int32),
            pltpu.SMEM((1, 128), jnp.int32),
            pltpu.VMEM((N_MP, 8, HEAD), F32),
            pltpu.VMEM((N_MP, 8, HEAD), F32),
            *[pltpu.VMEM((1, USERS), jnp.int32)] * 3,
            *[pltpu.SMEM((1, USERS), jnp.int32)] * 3,
            pltpu.VMEM((N_MP, GROUPS, LATE, TILE, HEAD), BF16),
            pltpu.VMEM((N_DP, LATE, TILE, HEAD), BF16),
            pltpu.VMEM((N_DP, LATE, TILE, HEAD), BF16),
        ]
        + [pltpu.VMEM((N_MP, GROUPS, part, TILE, HEAD), BF16) for part in PARTS]
        + [pltpu.VMEM((N_DP, part, TILE, HEAD), BF16) for part in PARTS * 3]
        + [
            dma((3,)), dma((6,)), dma((3,)), dma((3,)), dma((3,)), dma((3,)), dma, dma, dma((3,)), dma((3,)),
            *[dma((CHUNKS,))] * 6, dma((3,)), dma((3,)), dma,
            dma, dma, dma, dma, dma, dma, dma,
        ],
        compiler_params=pltpu.CompilerParams(collective_id=0, has_side_effects=True),
        name="layer_and_repack",
    )(
        tokens.reshape(BLK_DEV, BLOCK, D), w_uvqk, w_out,
        hist_len, owner, recv_offset, block_start,
    )
    packed, state = pl.pallas_call(
        unpack_kernel,
        out_shape=(
            jax.ShapeDtypeStruct((BLK_DEV * 8, TILE, HEAD), BF16),
            jax.ShapeDtypeStruct((USERS, HEAD), BF16),
        ),
        in_specs=[vmem, vmem, smem, vmem],
        out_specs=(vmem, vmem),
        name="unpack",
    )(landed, landed_early.reshape(N_MP, EARLY, GROUPS, TILE, HEAD), meta, states)
    return packed.reshape(BLK_DEV * BLOCK, HEAD), state


def solution(mesh):
    in_specs = (
        P("dp", None),
        P(None, "mp"),
        P(),
        P("dp", None),
        P("dp", None),
        P("dp", None),
        P("dp", None),
    )
    out_specs = (P("dp", "mp"), P("dp", "mp"))
    return jax.shard_map(
        per_device, mesh=mesh, in_specs=in_specs, out_specs=out_specs, check_vma=False
    )
```

```python
import functools

import jax
import jax.numpy as jnp
from jax import lax
from jax.experimental import pallas as pl
from jax.experimental.pallas import tpu as pltpu
from jax.sharding import PartitionSpec as P

D = 512
HEADS = 4
HEAD = 128
BLOCK = 128
WINDOW = 256
USERS = 24
BLK_DEV = 48
N_DP = 64
N_MP = 4
OWN = USERS // N_MP
PARTS = (2, 1)
EARLY = sum(PARTS)
CHUNKS = len(PARTS)
STARTS = tuple(sum(PARTS[:c]) for c in range(CHUNKS))
LATE = OWN - EARLY
TILE = 16
GROUPS = WINDOW // TILE
EPS = 1e-05
MESH = pl.DeviceIdType.MESH
BF16 = jnp.bfloat16
F32 = jnp.float32


def shift_of(i):
    return 2 * (i % 2) + (i // 2) % 2


def gated_silu(v):
    half = v * 0.5
    return half + half * jnp.tanh(half)


def main_kernel(
    tokens, w_in, w_out, len_in, own_in, off_in, start_in,
    landed, landed_early, meta, states,
    tok, wbuf, wo, normed, att, gates, x_early, mix_early, tab, build, pin_v, pin_s, st_send, st_recv,
    len_v, own_v, off_v, len_s, own_s, start_s, out_late, mid_late, pack_late, *rest,
):
    out_early, mid_early, pack_early, in_early = (
        rest[n * CHUNKS : (n + 1) * CHUNKS] for n in range(4)
    )
    (loc_sem, in_sem, w_send, w_recv, f_send, f_recv, t_send, t_recv, s_send, s_recv,
    e1_send, e1_recv, e1_loc, e2_send, e2_recv, e2_loc, x_send, x_recv, x_loc,
    l1_send, l1_recv, l1_loc, l2_send, l2_recv, l2_loc, pin_sem) = rest[4 * CHUNKS :]
    me = lax.axis_index("dp")
    mp = lax.axis_index("mp")
    core = me % 2
    partner = me + 1 - 2 * core
    right = (mp + 1) % N_MP
    left = (mp + 3) % N_MP
    across = (mp + 2) % N_MP

    load_tok = pltpu.make_async_copy(tokens, tok, loc_sem.at[0])
    load_tok.start()
    small = [
        pltpu.make_async_copy(src, dst, in_sem.at[n])
        for n, (src, dst) in enumerate(
            (
                (start_in, start_s), (len_in, len_v), (own_in, own_v), (off_in, off_v),
                (len_in, len_s), (own_in, own_s),
            )
        )
    ]
    load_w = pltpu.make_async_copy(w_in, wbuf.at[mp], loc_sem.at[1])
    load_wo = pltpu.make_async_copy(w_out, wo, loc_sem.at[2])
    for copy in small:
        copy.start()
    load_w.start()
    load_wo.start()

    barrier = pltpu.get_barrier_semaphore()

    def greet(peer):
        pl.semaphore_signal(barrier, inc=1, device_id=(peer % N_DP, mp), device_id_type=MESH)

    greet(me + N_DP // 2)

    @pl.loop(1, N_DP // 2)
    def _(t):
        greet(me + N_DP // 2 + t)
        greet(me + N_DP // 2 - t)

    for other in (right, left, across):
        pl.semaphore_signal(barrier, inc=1, device_id=(me, other), device_id_type=MESH)

    for copy in small:
        copy.wait()

    build[...] = jnp.zeros_like(build)
    build[0:1, 0:USERS] = len_v[...]
    build[1:2, 0:USERS] = own_v[...]
    build[2:3, 0:USERS] = off_v[...]
    tab[me] = (
        build[0:1]
        + pltpu.roll(build[1:2], USERS, 1)
        + pltpu.roll(build[2:3], 2 * USERS, 1)
    )
    st_send[...] = jnp.zeros_like(st_send)

    load_tok.wait()

    def user_blocks(k):
        start = start_s[0, mp * OWN + k]
        return tok[start], tok[jnp.minimum(start + 1, BLK_DEV - 1)]

    def user_rows(k):
        return jnp.concatenate(user_blocks(k), axis=0).astype(F32)

    for k in range(EARLY):
        for s, block in enumerate(user_blocks(k)):
            for q in range(N_MP):
                part = block[:, q * HEAD : (q + 1) * HEAD]
                c = sum(k >= low for low in STARTS) - 1
                out_early[c][q, s * 8 : s * 8 + 8, k - STARTS[c]] = part.reshape(8, TILE, HEAD)

    load_w.wait()
    pl.semaphore_wait(barrier, N_DP - 1 + N_MP - 1)

    half = pl.ds(pl.multiple_of(core * 256, 256), 256)

    def send_w(shard, target, k):
        return pltpu.make_async_remote_copy(
            src_ref=wbuf.at[shard, half], dst_ref=wbuf.at[shard, half],
            send_sem=w_send.at[k], recv_sem=w_recv.at[k],
            device_id=(me, target), device_id_type=MESH,
        )

    def forward_w(shard, k):
        return pltpu.make_async_remote_copy(
            src_ref=wbuf.at[shard, half], dst_ref=wbuf.at[shard, half],
            send_sem=f_send.at[k], recv_sem=f_recv.at[k],
            device_id=(partner, mp), device_id_type=MESH,
        )

    to_right = send_w(mp, right, 0)
    to_left = send_w(mp, left, 1)
    to_right.start()
    to_left.start()

    def send_tables():
        @pl.loop(1, N_DP)
        def _(t):
            pltpu.make_async_remote_copy(
                src_ref=tab.at[me], dst_ref=tab.at[me], send_sem=t_send, recv_sem=t_recv,
                device_id=((me + t) % N_DP, mp), device_id_type=MESH,
            ).start()

    own_early = []
    for c in range(CHUNKS):
        @pl.loop(1, N_DP)
        def _(t):
            i = (me + 27 * t) % N_DP
            pltpu.make_async_remote_copy(
                src_ref=out_early[c].at[i % 4, i // 4], dst_ref=mid_early[c].at[me],
                send_sem=e1_send.at[c], recv_sem=e1_recv.at[c],
                device_id=(i, mp), device_id_type=MESH,
            ).start()

        copy = pltpu.make_async_copy(
            out_early[c].at[me % 4, me // 4], mid_early[c].at[me], e1_loc.at[c]
        )
        copy.start()
        own_early.append(copy)
        if c == 0:
            send_tables()

    load_wo.wait()
    def normalize(k, x):
        mean = jnp.mean(x, axis=-1, keepdims=True)
        var = jnp.mean(x * x, axis=-1, keepdims=True) - mean * mean
        normed[k] = ((x - mean) * lax.rsqrt(var + EPS)).astype(BF16)

    @pl.loop(EARLY, OWN)
    def _(k):
        normalize(k, user_rows(k))

    row_id = lax.broadcasted_iota(jnp.int32, (BLOCK, BLOCK), 0)
    col_id = lax.broadcasted_iota(jnp.int32, (BLOCK, BLOCK), 1)
    causal = col_id <= row_id
    scaling = float(HEAD) ** -0.5
    nt = (((1,), (1,)), ((), ()))

    def head_of_user(shard, k):
        projected = gated_silu(
            jnp.dot(normed[k], wbuf[shard], preferred_element_type=F32)
        ).astype(BF16)
        gates[k, shard] = projected[:, 0:HEAD]
        v = projected[:, HEAD : 2 * HEAD]
        q = projected[:, 2 * HEAD : 3 * HEAD]
        key = projected[:, 3 * HEAD :]
        diag = jnp.concatenate(
            [
                lax.dot_general(q[:BLOCK], key[:BLOCK], nt, preferred_element_type=F32),
                lax.dot_general(q[BLOCK:], key[BLOCK:], nt, preferred_element_type=F32),
            ],
            axis=0,
        )
        back = lax.dot_general(q[BLOCK:], key[:BLOCK], nt, preferred_element_type=F32)
        both = jnp.concatenate([causal, causal], axis=0)
        w_diag = jnp.where(both, gated_silu(diag * scaling), 0.0).astype(BF16)
        w_back = gated_silu(back * scaling).astype(BF16)
        att[k, shard, 0:BLOCK] = jnp.dot(w_diag[:BLOCK], v[:BLOCK], preferred_element_type=F32)
        att[k, shard, BLOCK:] = jnp.dot(
            jnp.concatenate([w_back, w_diag[BLOCK:]], axis=1), v, preferred_element_type=F32
        )

    def heads(shard, low, high):
        @pl.loop(low, high)
        def _(k):
            head_of_user(shard, k)

    heads(mp, EARLY, OWN)

    def finish(k, x):
        a = [att[k, h] for h in range(HEADS)]
        total = sum(jnp.sum(p, axis=-1, keepdims=True) for p in a)
        squares = sum(jnp.sum(p * p, axis=-1, keepdims=True) for p in a)
        mean = total * (1.0 / D)
        var = squares * (1.0 / D) - mean * mean
        scale = lax.rsqrt(var + EPS * float(WINDOW * WINDOW))
        gated = jnp.concatenate(
            [((p - mean) * scale * gates[k, h].astype(F32)).astype(BF16) for h, p in enumerate(a)],
            axis=1,
        )
        mixed = jnp.dot(gated, wo[...], preferred_element_type=F32) + x
        return mixed

    def live_rows(mixed, count):
        rows = lax.broadcasted_iota(jnp.int32, (WINDOW, D), 0)
        return jnp.where(rows < count, mixed, 0.0).astype(BF16)

    def keep_state(k, mixed):
        last = len_s[0, mp * OWN + k] - 1
        rows = lax.broadcasted_iota(jnp.int32, (WINDOW, HEAD), 0)
        for q in range(N_MP):
            part = mixed[:, q * HEAD : (q + 1) * HEAD].astype(BF16).astype(F32)
            state = jnp.sum(jnp.where(rows == last, part, 0.0), axis=0, keepdims=True)
            st_send[q, pl.ds(k, 1)] = state

    to_right.wait_recv()
    from_left = forward_w(left, 0)
    from_left.start()
    to_left.wait_recv()
    from_right = forward_w(right, 1)
    from_right.start()
    onward_shard = jnp.where(core == 0, left, right)
    onward_target = jnp.where(core == 0, right, left)
    onward = send_w(onward_shard, onward_target, 2)
    onward.start()
    from_left.wait_recv()
    heads(left, EARLY, OWN)
    from_right.wait_recv()
    heads(right, EARLY, OWN)
    onward.wait_recv()
    from_across = forward_w(across, 2)
    from_across.start()
    from_across.wait_recv()

    @pl.loop(0, LATE)
    def _(j):
        k = EARLY + j
        head_of_user(across, k)
        mixed = finish(k, user_rows(k))
        keep_state(k, mixed)
        mixed = live_rows(mixed, len_s[0, mp * OWN + k])
        for q in range(N_MP):
            part = mixed[:, q * HEAD : (q + 1) * HEAD]
            out_late[q, :, j] = part.reshape(GROUPS, TILE, HEAD)

    def send_late(i, hop):
        column = (mp + hop) % N_MP
        pltpu.make_async_remote_copy(
            src_ref=out_late.at[column, i // 4], dst_ref=mid_late.at[me],
            send_sem=l1_send, recv_sem=l1_recv,
            device_id=(i, column), device_id_type=MESH,
        ).start()

    @pl.loop(1, N_DP)
    def _(t):
        i = (me + 27 * t) % N_DP
        send_late(i, shift_of(i))

    hop = shift_of(me)

    @pl.when(hop != 0)
    def _():
        send_late(me, hop)

    @pl.when(hop == 0)
    def _():
        pltpu.make_async_copy(out_late.at[mp, me // 4], mid_late.at[me], l1_loc).start()

    def wait_slots(ref, count, sem):
        some = ref.at[pl.ds(0, count)]
        pltpu.make_async_copy(some, some, sem).wait()

    wait_slots(tab, N_DP - 1, t_recv)
    rows = tab[...].reshape(N_DP, 128)
    owners = pltpu.roll(rows, 128 - USERS, 1)
    offsets = pltpu.roll(rows, 128 - 2 * USERS, 1)
    lane = lax.broadcasted_iota(jnp.int32, (N_DP, 128), 1)
    source = lax.broadcasted_iota(jnp.int32, (N_DP, 128), 0)

    def pick(mask, values):
        return jnp.max(jnp.where(mask, values, 0), axis=0, keepdims=True)

    pin = pick(owners[:, 0:1] == lane, source)
    lens = pick(owners == me, rows)
    offs = pick(owners == me, offsets)
    pin_v[...] = jnp.zeros((8, 128), jnp.int32)
    pin_v[0:1] = pin
    pin_v[1:2] = lens
    meta[...] = jnp.zeros((8, 128), jnp.int32)
    meta[0:1] = lens
    meta[1:2] = offs
    to_scalars = pltpu.make_async_copy(pin_v, pin_s, pin_sem)
    to_scalars.start()
    to_scalars.wait()

    def regroup(packed, middle, low, count):
        firsts = [own_s[0, low + j] - own_s[0, 0] for j in range(count)]

        @pl.loop(0, N_DP, unroll=4)
        def _(o):
            for j in range(count):
                packed[o, j] = middle[pin_s[0, (o - firsts[j]) & (N_DP - 1)], j]

    kept_early = []
    for c in range(CHUNKS):
        wait_slots(mid_early[c], N_DP - 1, e1_recv.at[c])
        own_early[c].wait()
        regroup(pack_early[c], mid_early[c], mp * OWN + STARTS[c], PARTS[c])

        @pl.loop(1, N_DP)
        def _(t):
            o = (me + 27 * t) % N_DP
            pltpu.make_async_remote_copy(
                src_ref=pack_early[c].at[o], dst_ref=in_early[c].at[me],
                send_sem=e2_send.at[c], recv_sem=e2_recv.at[c],
                device_id=(o, mp), device_id_type=MESH,
            ).start()

        copy = pltpu.make_async_copy(pack_early[c].at[me], in_early[c].at[me], e2_loc.at[c])
        copy.start()
        kept_early.append(copy)

    @pl.loop(0, EARLY)
    def _(k):
        normalize(k, user_rows(k))

    for shard in (mp, left, right):
        heads(shard, 0, EARLY)

    @pl.loop(0, EARLY)
    def _(k):
        head_of_user(across, k)
        keep_state(k, finish(k, user_rows(k)))

    state_copies = []
    for n, (other, source) in enumerate(((right, left), (left, right), (across, across))):
        copy = pltpu.make_async_remote_copy(
            src_ref=st_send.at[other], dst_ref=st_recv.at[mp],
            send_sem=s_send.at[n], recv_sem=s_recv.at[n],
            device_id=(me, other), device_id_type=MESH,
        )
        copy.start()
        state_copies.append(copy)

    @pl.when(hop != 0)
    def _():
        wait_slots(mid_late, N_DP, l1_recv)

    @pl.when(hop == 0)
    def _():
        wait_slots(mid_late, N_DP - 1, l1_recv)
        pltpu.make_async_copy(out_late.at[mp, me // 4], mid_late.at[me], l1_loc).wait()

    regroup(pack_late, mid_late, (mp - hop + N_MP) % N_MP * OWN + EARLY, LATE)

    @pl.loop(1, N_DP)
    def _(t):
        o = (me + 27 * t) % N_DP
        pltpu.make_async_remote_copy(
            src_ref=pack_late.at[o], dst_ref=landed.at[me],
            send_sem=l2_send, recv_sem=l2_recv,
            device_id=(o, mp), device_id_type=MESH,
        ).start()

    kept_late = pltpu.make_async_copy(pack_late.at[me], landed.at[me], l2_loc)
    kept_late.start()

    for c in range(CHUNKS):
        wait_slots(in_early[c], N_DP - 1, e2_recv.at[c])
        kept_early[c].wait()
        mine = range(STARTS[c], STARTS[c] + PARTS[c])

        @pl.loop(0, GROUPS)
        def _(g):
            rows = pl.ds(pl.multiple_of(g * TILE, TILE), TILE)
            for q in range(N_MP):
                for k in mine:
                    x_early[k, rows, q * HEAD : (q + 1) * HEAD] = in_early[c][4 * g + q, k - STARTS[c]]

        for k in mine:
            normalize(k, x_early[k].astype(F32))

        for shard in (mp, left, right):
            heads(shard, mine[0], mine[0] + PARTS[c])

        @pl.loop(mine[0], mine[0] + PARTS[c])
        def _(k):
            head_of_user(across, k)
            mixed = live_rows(finish(k, x_early[k].astype(F32)), pin_s[1, mp * OWN + k])
            for q in range(N_MP):
                mix_early[q, k] = mixed[:, q * HEAD : (q + 1) * HEAD]
            for n, other in enumerate((right, left, across)):
                pltpu.make_async_remote_copy(
                    src_ref=mix_early.at[other, k], dst_ref=landed_early.at[mp, k],
                    send_sem=x_send.at[n], recv_sem=x_recv.at[n],
                    device_id=(me, other), device_id_type=MESH,
                ).start()

    kept = pltpu.make_async_copy(mix_early.at[mp], landed_early.at[mp], x_loc)
    kept.start()

    for copy in state_copies:
        copy.wait()
    for m in range(N_MP):
        @pl.when(m != mp)
        def _():
            states[m] = st_recv[m]

        @pl.when(m == mp)
        def _():
            states[m] = st_send[m]

    for copy in (to_right, to_left, onward, from_left, from_right, from_across):
        copy.wait_send()
    wait_slots(tab, N_DP - 1, t_send)
    for c in range(CHUNKS):
        wait_slots(mid_early[c], N_DP - 1, e1_send.at[c])
        wait_slots(mid_early[c], N_DP - 1, e2_send.at[c])

    @pl.when(hop != 0)
    def _():
        wait_slots(mid_late, N_DP, l1_send)

    @pl.when(hop == 0)
    def _():
        wait_slots(mid_late, N_DP - 1, l1_send)

    wait_slots(mid_late, N_DP - 1, l2_send)
    for n, (other, source) in enumerate(((right, left), (left, right), (across, across))):
        pltpu.make_async_remote_copy(
            src_ref=mix_early.at[other], dst_ref=landed_early.at[source],
            send_sem=x_send.at[n], recv_sem=x_recv.at[n],
            device_id=(me, other), device_id_type=MESH,
        ).wait()
    kept.wait()

    wait_slots(mid_late, N_DP - 1, l2_recv)
    kept_late.wait()


def unpack_kernel(landed, landed_early, meta, states, out, state_out, zeros, block_of, sem):
    mp = lax.axis_index("mp")
    zeros[...] = jnp.zeros_like(zeros)

    @pl.loop(0, BLK_DEV, unroll=8)
    def _(b):
        block_of[0, b] = -1

    for m in range(N_MP):
        for k in range(OWN):
            u = m * OWN + k
            code = (m * 8 + k) * 2
            first = meta[1, u]
            block_of[0, first] = code

            @pl.when(meta[0, u] > BLOCK)
            def _():
                block_of[0, first + 1] = code + 1

    @pl.loop(0, BLK_DEV)
    def _(b):
        code = block_of[0, b]
        m = (code >> 4) & 3
        k = (code >> 1) & 7
        groups = pl.ds((code & 1) * 8, 8)

        @pl.when(code < 0)
        def _():
            pltpu.make_async_copy(zeros, out.at[b], sem).start()

        @pl.when((code >= 0) & (k < EARLY))
        def _():
            pltpu.make_async_copy(landed_early.at[m, k, groups], out.at[b], sem).start()

        @pl.when((code >= 0) & (k >= EARLY))
        def _():
            delta = (mp - m) & 3
            low = (delta >> 1) + 2 * (delta & 1)
            pltpu.make_async_copy(landed.at[groups, low, k - EARLY], out.at[b], sem).start()

    for m in range(N_MP):
        for k in range(OWN):
            state_out[pl.ds(m * OWN + k, 1)] = states[m, pl.ds(k, 1)].astype(BF16)
    pltpu.make_async_copy(out, out, sem).wait()


def per_device(tokens, w_uvqk, w_out, hist_len, owner, recv_offset, block_start):
    any_spec = pl.BlockSpec(memory_space=pl.ANY)
    vmem = pl.BlockSpec(memory_space=pltpu.VMEM)
    smem = pl.BlockSpec(memory_space=pltpu.SMEM)
    dma = pltpu.SemaphoreType.DMA
    landed, landed_early, meta, states = pl.pallas_call(
        main_kernel,
        out_shape=(
            jax.ShapeDtypeStruct((N_DP, LATE, TILE, HEAD), BF16),
            jax.ShapeDtypeStruct((N_MP, EARLY, WINDOW, HEAD), BF16),
            jax.ShapeDtypeStruct((8, 128), jnp.int32),
            jax.ShapeDtypeStruct((N_MP, 8, HEAD), F32),
        ),
        in_specs=[any_spec] * 7,
        out_specs=(any_spec, any_spec, vmem, vmem),
        scratch_shapes=[
            pltpu.VMEM((BLK_DEV, BLOCK, D), BF16),
            pltpu.VMEM((N_MP, D, D), BF16),
            pltpu.VMEM((D, D), BF16),
            pltpu.VMEM((OWN, WINDOW, D), BF16),
            pltpu.VMEM((OWN, HEADS, WINDOW, HEAD), F32),
            pltpu.VMEM((OWN, HEADS, WINDOW, HEAD), BF16),
            pltpu.VMEM((EARLY, WINDOW, D), BF16),
            pltpu.VMEM((N_MP, EARLY, WINDOW, HEAD), BF16),
            pltpu.VMEM((N_DP, 1, 128), jnp.int32),
            pltpu.VMEM((8, 128), jnp.int32),
            pltpu.VMEM((8, 128), jnp.int32),
            pltpu.SMEM((8, 128), jnp.int32),
            pltpu.VMEM((N_MP, 8, HEAD), F32),
            pltpu.VMEM((N_MP, 8, HEAD), F32),
            *[pltpu.VMEM((1, USERS), jnp.int32)] * 3,
            *[pltpu.SMEM((1, USERS), jnp.int32)] * 3,
            pltpu.VMEM((N_MP, GROUPS, LATE, TILE, HEAD), BF16),
            pltpu.VMEM((N_DP, LATE, TILE, HEAD), BF16),
            pltpu.VMEM((N_DP, LATE, TILE, HEAD), BF16),
        ]
        + [pltpu.VMEM((N_MP, GROUPS, part, TILE, HEAD), BF16) for part in PARTS]
        + [pltpu.VMEM((N_DP, part, TILE, HEAD), BF16) for part in PARTS * 3]
        + [
            dma((3,)), dma((6,)), dma((3,)), dma((3,)), dma((3,)), dma((3,)), dma, dma, dma((3,)), dma((3,)),
            *[dma((CHUNKS,))] * 6, dma((3,)), dma((3,)), dma,
            dma, dma, dma, dma, dma, dma, dma,
        ],
        compiler_params=pltpu.CompilerParams(
            collective_id=0, has_side_effects=True, vmem_limit_bytes=40 * 2**20
        ),
        name="layer_and_repack",
    )(
        *(
            pltpu.with_memory_space_constraint(a, pltpu.HBM)
            for a in (
                tokens.reshape(BLK_DEV, BLOCK, D), w_uvqk, w_out,
                hist_len, owner, recv_offset, block_start,
            )
        )
    )
    packed, state = pl.pallas_call(
        unpack_kernel,
        out_shape=(
            jax.ShapeDtypeStruct((BLK_DEV, 8, TILE, HEAD), BF16),
            jax.ShapeDtypeStruct((USERS, HEAD), BF16),
        ),
        in_specs=[any_spec, any_spec, smem, vmem],
        out_specs=(any_spec, vmem),
        scratch_shapes=[pltpu.VMEM((8, TILE, HEAD), BF16), pltpu.SMEM((1, 128), jnp.int32), dma],
        compiler_params=pltpu.CompilerParams(vmem_limit_bytes=16 * 2**20),
        name="unpack",
    )(
        landed.reshape(GROUPS, N_MP, LATE, TILE, HEAD),
        landed_early.reshape(N_MP, EARLY, GROUPS, TILE, HEAD),
        meta, states,
    )
    return packed.reshape(BLK_DEV * BLOCK, HEAD), state


def solution(mesh):
    in_specs = (
        P("dp", None),
        P(None, "mp"),
        P(),
        P("dp", None),
        P("dp", None),
        P("dp", None),
        P("dp", None),
    )
    out_specs = (P("dp", "mp"), P("dp", "mp"))
    return jax.shard_map(
        per_device, mesh=mesh, in_specs=in_specs, out_specs=out_specs, check_vma=False
    )
```

```python
import functools

import jax
import jax.numpy as jnp
from jax import lax
from jax.experimental import pallas as pl
from jax.experimental.pallas import tpu as pltpu
from jax.sharding import PartitionSpec as P

D = 512
HEADS = 4
HEAD = 128
BLOCK = 128
WINDOW = 256
USERS = 24
BLK_DEV = 48
N_DP = 64
N_MP = 4
OWN = USERS // N_MP
PARTS = (1, 2)
EARLY = sum(PARTS)
CHUNKS = len(PARTS)
STARTS = tuple(sum(PARTS[:c]) for c in range(CHUNKS))
LATE = OWN - EARLY
TILE = 16
GROUPS = WINDOW // TILE
EPS = 1e-05
MESH = pl.DeviceIdType.MESH
BF16 = jnp.bfloat16
F32 = jnp.float32


def shift_of(i):
    return 2 * (i % 2) + (i // 2) % 2


def gated_silu(v):
    half = v * 0.5
    return half + half * jnp.tanh(half)


def main_kernel(
    tokens, w_in, w_out, len_in, own_in, off_in, start_in,
    landed, landed_early, meta, states,
    tok, wbuf, wo, normed, att, gates, x_early, mix_early, tab, build, pin_v, pin_s, st_send, st_recv,
    len_v, own_v, off_v, len_s, own_s, start_s, out_late, mid_late, pack_late, *rest,
):
    out_early, mid_early, pack_early, in_early = (
        rest[n * CHUNKS : (n + 1) * CHUNKS] for n in range(4)
    )
    (loc_sem, in_sem, w_send, w_recv, f_send, f_recv, t_send, t_recv, s_send, s_recv,
    e1_send, e1_recv, e1_loc, e2_send, e2_recv, e2_loc, x_send, x_recv, x_loc,
    l1_send, l1_recv, l1_loc, l2_send, l2_recv, l2_loc, pin_sem) = rest[4 * CHUNKS :]
    me = lax.axis_index("dp")
    mp = lax.axis_index("mp")
    core = me % 2
    partner = me + 1 - 2 * core
    right = (mp + 1) % N_MP
    left = (mp + 3) % N_MP
    across = (mp + 2) % N_MP

    load_tok = pltpu.make_async_copy(tokens, tok, loc_sem.at[0])
    load_tok.start()
    small = [
        pltpu.make_async_copy(src, dst, in_sem.at[n])
        for n, (src, dst) in enumerate(
            (
                (start_in, start_s), (len_in, len_v), (own_in, own_v), (off_in, off_v),
                (len_in, len_s), (own_in, own_s),
            )
        )
    ]
    load_w = pltpu.make_async_copy(w_in, wbuf.at[mp], loc_sem.at[1])
    load_wo = pltpu.make_async_copy(w_out, wo, loc_sem.at[2])
    for copy in small:
        copy.start()
    load_w.start()
    load_wo.start()

    barrier = pltpu.get_barrier_semaphore()

    def greet(peer):
        pl.semaphore_signal(barrier, inc=1, device_id=(peer % N_DP, mp), device_id_type=MESH)

    greet(me + N_DP // 2)

    @pl.loop(1, N_DP // 2)
    def _(t):
        greet(me + N_DP // 2 + t)
        greet(me + N_DP // 2 - t)

    for other in (right, left, across):
        pl.semaphore_signal(barrier, inc=1, device_id=(me, other), device_id_type=MESH)

    for copy in small:
        copy.wait()

    build[...] = jnp.zeros_like(build)
    build[0:1, 0:USERS] = len_v[...]
    build[1:2, 0:USERS] = own_v[...]
    build[2:3, 0:USERS] = off_v[...]
    tab[me] = (
        build[0:1]
        + pltpu.roll(build[1:2], USERS, 1)
        + pltpu.roll(build[2:3], 2 * USERS, 1)
    )
    st_send[...] = jnp.zeros_like(st_send)

    load_tok.wait()

    def user_blocks(k):
        start = start_s[0, mp * OWN + k]
        return tok[start], tok[jnp.minimum(start + 1, BLK_DEV - 1)]

    def user_rows(k):
        return jnp.concatenate(user_blocks(k), axis=0).astype(F32)

    for k in range(EARLY):
        for s, block in enumerate(user_blocks(k)):
            for q in range(N_MP):
                part = block[:, q * HEAD : (q + 1) * HEAD]
                c = sum(k >= low for low in STARTS) - 1
                out_early[c][q, s * 8 : s * 8 + 8, k - STARTS[c]] = part.reshape(8, TILE, HEAD)

    load_w.wait()
    pl.semaphore_wait(barrier, N_DP - 1 + N_MP - 1)

    half = pl.ds(pl.multiple_of(core * 256, 256), 256)

    def send_w(shard, target, k):
        return pltpu.make_async_remote_copy(
            src_ref=wbuf.at[shard, half], dst_ref=wbuf.at[shard, half],
            send_sem=w_send.at[k], recv_sem=w_recv.at[k],
            device_id=(me, target), device_id_type=MESH,
        )

    def forward_w(shard, k):
        return pltpu.make_async_remote_copy(
            src_ref=wbuf.at[shard, half], dst_ref=wbuf.at[shard, half],
            send_sem=f_send.at[k], recv_sem=f_recv.at[k],
            device_id=(partner, mp), device_id_type=MESH,
        )

    to_right = send_w(mp, right, 0)
    to_left = send_w(mp, left, 1)
    to_right.start()
    to_left.start()

    def send_tables():
        @pl.loop(1, N_DP)
        def _(t):
            pltpu.make_async_remote_copy(
                src_ref=tab.at[me], dst_ref=tab.at[me], send_sem=t_send, recv_sem=t_recv,
                device_id=((me + t) % N_DP, mp), device_id_type=MESH,
            ).start()

    own_early = []
    for c in range(CHUNKS):
        @pl.loop(1, N_DP)
        def _(t):
            i = (me + 27 * t) % N_DP
            pltpu.make_async_remote_copy(
                src_ref=out_early[c].at[i % 4, i // 4], dst_ref=mid_early[c].at[me],
                send_sem=e1_send.at[c], recv_sem=e1_recv.at[c],
                device_id=(i, mp), device_id_type=MESH,
            ).start()

        copy = pltpu.make_async_copy(
            out_early[c].at[me % 4, me // 4], mid_early[c].at[me], e1_loc.at[c]
        )
        copy.start()
        own_early.append(copy)
        if c == 0:
            send_tables()

    load_wo.wait()
    def normalize(k, x):
        mean = jnp.mean(x, axis=-1, keepdims=True)
        var = jnp.mean(x * x, axis=-1, keepdims=True) - mean * mean
        normed[k] = ((x - mean) * lax.rsqrt(var + EPS)).astype(BF16)

    @pl.loop(EARLY, OWN)
    def _(k):
        normalize(k, user_rows(k))

    row_id = lax.broadcasted_iota(jnp.int32, (BLOCK, BLOCK), 0)
    col_id = lax.broadcasted_iota(jnp.int32, (BLOCK, BLOCK), 1)
    causal = col_id <= row_id
    scaling = float(HEAD) ** -0.5
    nt = (((1,), (1,)), ((), ()))

    def head_of_user(shard, k):
        projected = gated_silu(
            jnp.dot(normed[k], wbuf[shard], preferred_element_type=F32)
        ).astype(BF16)
        gates[k, shard] = projected[:, 0:HEAD]
        v = projected[:, HEAD : 2 * HEAD]
        q = projected[:, 2 * HEAD : 3 * HEAD]
        key = projected[:, 3 * HEAD :]
        diag = jnp.concatenate(
            [
                lax.dot_general(q[:BLOCK], key[:BLOCK], nt, preferred_element_type=F32),
                lax.dot_general(q[BLOCK:], key[BLOCK:], nt, preferred_element_type=F32),
            ],
            axis=0,
        )
        back = lax.dot_general(q[BLOCK:], key[:BLOCK], nt, preferred_element_type=F32)
        both = jnp.concatenate([causal, causal], axis=0)
        w_diag = jnp.where(both, gated_silu(diag * scaling), 0.0).astype(BF16)
        w_back = gated_silu(back * scaling).astype(BF16)
        att[k, shard, 0:BLOCK] = jnp.dot(w_diag[:BLOCK], v[:BLOCK], preferred_element_type=F32)
        att[k, shard, BLOCK:] = jnp.dot(
            jnp.concatenate([w_back, w_diag[BLOCK:]], axis=1), v, preferred_element_type=F32
        )

    def heads(shard, low, high):
        @pl.loop(low, high)
        def _(k):
            head_of_user(shard, k)

    heads(mp, EARLY, OWN)

    def finish(k, x):
        a = [att[k, h] for h in range(HEADS)]
        total = sum(jnp.sum(p, axis=-1, keepdims=True) for p in a)
        squares = sum(jnp.sum(p * p, axis=-1, keepdims=True) for p in a)
        mean = total * (1.0 / D)
        var = squares * (1.0 / D) - mean * mean
        scale = lax.rsqrt(var + EPS * float(WINDOW * WINDOW))
        gated = jnp.concatenate(
            [((p - mean) * scale * gates[k, h].astype(F32)).astype(BF16) for h, p in enumerate(a)],
            axis=1,
        )
        mixed = jnp.dot(gated, wo[...], preferred_element_type=F32) + x
        return mixed

    def live_rows(mixed, count):
        rows = lax.broadcasted_iota(jnp.int32, (WINDOW, D), 0)
        return jnp.where(rows < count, mixed, 0.0).astype(BF16)

    def keep_state(k, mixed):
        last = len_s[0, mp * OWN + k] - 1
        rows = lax.broadcasted_iota(jnp.int32, (WINDOW, HEAD), 0)
        for q in range(N_MP):
            part = mixed[:, q * HEAD : (q + 1) * HEAD].astype(BF16).astype(F32)
            state = jnp.sum(jnp.where(rows == last, part, 0.0), axis=0, keepdims=True)
            st_send[q, pl.ds(k, 1)] = state

    to_right.wait_recv()
    from_left = forward_w(left, 0)
    from_left.start()
    to_left.wait_recv()
    from_right = forward_w(right, 1)
    from_right.start()
    onward_shard = jnp.where(core == 0, left, right)
    onward_target = jnp.where(core == 0, right, left)
    onward = send_w(onward_shard, onward_target, 2)
    onward.start()
    from_left.wait_recv()
    heads(left, EARLY, OWN)
    from_right.wait_recv()
    heads(right, EARLY, OWN)
    def wait_slots(ref, count, sem):
        some = ref.at[pl.ds(0, count)]
        pltpu.make_async_copy(some, some, sem).wait()

    wait_slots(tab, N_DP - 1, t_recv)
    rows = tab[...].reshape(N_DP, 128)
    owners = pltpu.roll(rows, 128 - USERS, 1)
    offsets = pltpu.roll(rows, 128 - 2 * USERS, 1)
    lane = lax.broadcasted_iota(jnp.int32, (N_DP, 128), 1)
    source = lax.broadcasted_iota(jnp.int32, (N_DP, 128), 0)

    def pick(mask, values):
        return jnp.max(jnp.where(mask, values, 0), axis=0, keepdims=True)

    pin = pick(owners[:, 0:1] == lane, source)
    lens = pick(owners == me, rows)
    offs = pick(owners == me, offsets)
    pin_v[...] = jnp.zeros((8, 128), jnp.int32)
    pin_v[0:1] = pin
    pin_v[1:2] = lens
    meta[...] = jnp.zeros((8, 128), jnp.int32)
    meta[0:1] = lens
    meta[1:2] = offs
    to_scalars = pltpu.make_async_copy(pin_v, pin_s, pin_sem)
    to_scalars.start()
    to_scalars.wait()

    def regroup(packed, middle, low, count):
        firsts = [own_s[0, low + j] - own_s[0, 0] for j in range(count)]

        @pl.loop(0, N_DP, unroll=4)
        def _(o):
            for j in range(count):
                packed[o, j] = middle[pin_s[0, (o - firsts[j]) & (N_DP - 1)], j]

    kept_early = []

    def second_of_early(c):
        wait_slots(mid_early[c], N_DP - 1, e1_recv.at[c])
        own_early[c].wait()
        regroup(pack_early[c], mid_early[c], mp * OWN + STARTS[c], PARTS[c])

        @pl.loop(1, N_DP)
        def _(t):
            o = (me + 27 * t) % N_DP
            pltpu.make_async_remote_copy(
                src_ref=pack_early[c].at[o], dst_ref=in_early[c].at[me],
                send_sem=e2_send.at[c], recv_sem=e2_recv.at[c],
                device_id=(o, mp), device_id_type=MESH,
            ).start()

        copy = pltpu.make_async_copy(pack_early[c].at[me], in_early[c].at[me], e2_loc.at[c])
        copy.start()
        kept_early.append(copy)

    onward.wait_recv()
    from_across = forward_w(across, 2)
    from_across.start()
    second_of_early(0)
    from_across.wait_recv()

    @pl.loop(0, LATE)
    def _(j):
        k = EARLY + j
        head_of_user(across, k)
        mixed = finish(k, user_rows(k))
        keep_state(k, mixed)
        mixed = live_rows(mixed, len_s[0, mp * OWN + k])
        for q in range(N_MP):
            part = mixed[:, q * HEAD : (q + 1) * HEAD]
            out_late[q, :, j] = part.reshape(GROUPS, TILE, HEAD)

    def send_late(i, hop):
        column = (mp + hop) % N_MP
        pltpu.make_async_remote_copy(
            src_ref=out_late.at[column, i // 4], dst_ref=mid_late.at[me],
            send_sem=l1_send, recv_sem=l1_recv,
            device_id=(i, column), device_id_type=MESH,
        ).start()

    @pl.loop(1, N_DP)
    def _(t):
        i = (me + 27 * t) % N_DP
        send_late(i, shift_of(i))

    hop = shift_of(me)

    @pl.when(hop != 0)
    def _():
        send_late(me, hop)

    @pl.when(hop == 0)
    def _():
        pltpu.make_async_copy(out_late.at[mp, me // 4], mid_late.at[me], l1_loc).start()

    for c in range(1, CHUNKS):
        second_of_early(c)

    @pl.loop(0, EARLY)
    def _(k):
        normalize(k, user_rows(k))

    for shard in (mp, left, right):
        heads(shard, 0, EARLY)

    @pl.loop(0, EARLY)
    def _(k):
        head_of_user(across, k)
        keep_state(k, finish(k, user_rows(k)))

    state_copies = []
    for n, (other, source) in enumerate(((right, left), (left, right), (across, across))):
        copy = pltpu.make_async_remote_copy(
            src_ref=st_send.at[other], dst_ref=st_recv.at[mp],
            send_sem=s_send.at[n], recv_sem=s_recv.at[n],
            device_id=(me, other), device_id_type=MESH,
        )
        copy.start()
        state_copies.append(copy)

    @pl.when(hop != 0)
    def _():
        wait_slots(mid_late, N_DP, l1_recv)

    @pl.when(hop == 0)
    def _():
        wait_slots(mid_late, N_DP - 1, l1_recv)
        pltpu.make_async_copy(out_late.at[mp, me // 4], mid_late.at[me], l1_loc).wait()

    regroup(pack_late, mid_late, (mp - hop + N_MP) % N_MP * OWN + EARLY, LATE)

    @pl.loop(1, N_DP)
    def _(t):
        o = (me + 27 * t) % N_DP
        pltpu.make_async_remote_copy(
            src_ref=pack_late.at[o], dst_ref=landed.at[me],
            send_sem=l2_send, recv_sem=l2_recv,
            device_id=(o, mp), device_id_type=MESH,
        ).start()

    kept_late = pltpu.make_async_copy(pack_late.at[me], landed.at[me], l2_loc)
    kept_late.start()

    for c in range(CHUNKS):
        wait_slots(in_early[c], N_DP - 1, e2_recv.at[c])
        kept_early[c].wait()
        mine = range(STARTS[c], STARTS[c] + PARTS[c])

        @pl.loop(0, GROUPS)
        def _(g):
            rows = pl.ds(pl.multiple_of(g * TILE, TILE), TILE)
            for q in range(N_MP):
                for k in mine:
                    x_early[k, rows, q * HEAD : (q + 1) * HEAD] = in_early[c][4 * g + q, k - STARTS[c]]

        for k in mine:
            normalize(k, x_early[k].astype(F32))

        for shard in (mp, left, right):
            heads(shard, mine[0], mine[0] + PARTS[c])

        @pl.loop(mine[0], mine[0] + PARTS[c])
        def _(k):
            head_of_user(across, k)
            mixed = live_rows(finish(k, x_early[k].astype(F32)), pin_s[1, mp * OWN + k])
            for q in range(N_MP):
                mix_early[q, k] = mixed[:, q * HEAD : (q + 1) * HEAD]
            for n, other in enumerate((right, left, across)):
                pltpu.make_async_remote_copy(
                    src_ref=mix_early.at[other, k], dst_ref=landed_early.at[mp, k],
                    send_sem=x_send.at[n], recv_sem=x_recv.at[n],
                    device_id=(me, other), device_id_type=MESH,
                ).start()

    kept = pltpu.make_async_copy(mix_early.at[mp], landed_early.at[mp], x_loc)
    kept.start()

    for copy in state_copies:
        copy.wait()
    for m in range(N_MP):
        @pl.when(m != mp)
        def _():
            states[m] = st_recv[m]

        @pl.when(m == mp)
        def _():
            states[m] = st_send[m]

    for copy in (to_right, to_left, onward, from_left, from_right, from_across):
        copy.wait_send()
    wait_slots(tab, N_DP - 1, t_send)
    for c in range(CHUNKS):
        wait_slots(mid_early[c], N_DP - 1, e1_send.at[c])
        wait_slots(mid_early[c], N_DP - 1, e2_send.at[c])

    @pl.when(hop != 0)
    def _():
        wait_slots(mid_late, N_DP, l1_send)

    @pl.when(hop == 0)
    def _():
        wait_slots(mid_late, N_DP - 1, l1_send)

    wait_slots(mid_late, N_DP - 1, l2_send)
    for n, (other, source) in enumerate(((right, left), (left, right), (across, across))):
        pltpu.make_async_remote_copy(
            src_ref=mix_early.at[other], dst_ref=landed_early.at[source],
            send_sem=x_send.at[n], recv_sem=x_recv.at[n],
            device_id=(me, other), device_id_type=MESH,
        ).wait()
    kept.wait()

    wait_slots(mid_late, N_DP - 1, l2_recv)
    kept_late.wait()


def unpack_kernel(landed, landed_early, meta, states, out, state_out, zeros, block_of, sem):
    mp = lax.axis_index("mp")
    zeros[...] = jnp.zeros_like(zeros)

    @pl.loop(0, BLK_DEV, unroll=8)
    def _(b):
        block_of[0, b] = -1

    for m in range(N_MP):
        for k in range(OWN):
            u = m * OWN + k
            code = (m * 8 + k) * 2
            first = meta[1, u]
            block_of[0, first] = code

            @pl.when(meta[0, u] > BLOCK)
            def _():
                block_of[0, first + 1] = code + 1

    @pl.loop(0, BLK_DEV)
    def _(b):
        code = block_of[0, b]
        m = (code >> 4) & 3
        k = (code >> 1) & 7
        groups = pl.ds((code & 1) * 8, 8)

        @pl.when(code < 0)
        def _():
            pltpu.make_async_copy(zeros, out.at[b], sem).start()

        @pl.when((code >= 0) & (k < EARLY))
        def _():
            pltpu.make_async_copy(landed_early.at[m, k, groups], out.at[b], sem).start()

        @pl.when((code >= 0) & (k >= EARLY))
        def _():
            delta = (mp - m) & 3
            low = (delta >> 1) + 2 * (delta & 1)
            pltpu.make_async_copy(landed.at[groups, low, k - EARLY], out.at[b], sem).start()

    for m in range(N_MP):
        for k in range(OWN):
            state_out[pl.ds(m * OWN + k, 1)] = states[m, pl.ds(k, 1)].astype(BF16)
    pltpu.make_async_copy(out, out, sem).wait()


def per_device(tokens, w_uvqk, w_out, hist_len, owner, recv_offset, block_start):
    any_spec = pl.BlockSpec(memory_space=pl.ANY)
    vmem = pl.BlockSpec(memory_space=pltpu.VMEM)
    smem = pl.BlockSpec(memory_space=pltpu.SMEM)
    dma = pltpu.SemaphoreType.DMA
    landed, landed_early, meta, states = pl.pallas_call(
        main_kernel,
        out_shape=(
            jax.ShapeDtypeStruct((N_DP, LATE, TILE, HEAD), BF16),
            jax.ShapeDtypeStruct((N_MP, EARLY, WINDOW, HEAD), BF16),
            jax.ShapeDtypeStruct((8, 128), jnp.int32),
            jax.ShapeDtypeStruct((N_MP, 8, HEAD), F32),
        ),
        in_specs=[any_spec] * 7,
        out_specs=(any_spec, any_spec, vmem, vmem),
        scratch_shapes=[
            pltpu.VMEM((BLK_DEV, BLOCK, D), BF16),
            pltpu.VMEM((N_MP, D, D), BF16),
            pltpu.VMEM((D, D), BF16),
            pltpu.VMEM((OWN, WINDOW, D), BF16),
            pltpu.VMEM((OWN, HEADS, WINDOW, HEAD), F32),
            pltpu.VMEM((OWN, HEADS, WINDOW, HEAD), BF16),
            pltpu.VMEM((EARLY, WINDOW, D), BF16),
            pltpu.VMEM((N_MP, EARLY, WINDOW, HEAD), BF16),
            pltpu.VMEM((N_DP, 1, 128), jnp.int32),
            pltpu.VMEM((8, 128), jnp.int32),
            pltpu.VMEM((8, 128), jnp.int32),
            pltpu.SMEM((8, 128), jnp.int32),
            pltpu.VMEM((N_MP, 8, HEAD), F32),
            pltpu.VMEM((N_MP, 8, HEAD), F32),
            *[pltpu.VMEM((1, USERS), jnp.int32)] * 3,
            *[pltpu.SMEM((1, USERS), jnp.int32)] * 3,
            pltpu.VMEM((N_MP, GROUPS, LATE, TILE, HEAD), BF16),
            pltpu.VMEM((N_DP, LATE, TILE, HEAD), BF16),
            pltpu.VMEM((N_DP, LATE, TILE, HEAD), BF16),
        ]
        + [pltpu.VMEM((N_MP, GROUPS, part, TILE, HEAD), BF16) for part in PARTS]
        + [pltpu.VMEM((N_DP, part, TILE, HEAD), BF16) for part in PARTS * 3]
        + [
            dma((3,)), dma((6,)), dma((3,)), dma((3,)), dma((3,)), dma((3,)), dma, dma, dma((3,)), dma((3,)),
            *[dma((CHUNKS,))] * 6, dma((3,)), dma((3,)), dma,
            dma, dma, dma, dma, dma, dma, dma,
        ],
        compiler_params=pltpu.CompilerParams(
            collective_id=0, has_side_effects=True, vmem_limit_bytes=40 * 2**20
        ),
        name="layer_and_repack",
    )(
        *(
            pltpu.with_memory_space_constraint(a, pltpu.HBM)
            for a in (
                tokens.reshape(BLK_DEV, BLOCK, D), w_uvqk, w_out,
                hist_len, owner, recv_offset, block_start,
            )
        )
    )
    packed, state = pl.pallas_call(
        unpack_kernel,
        out_shape=(
            jax.ShapeDtypeStruct((BLK_DEV, 8, TILE, HEAD), BF16),
            jax.ShapeDtypeStruct((USERS, HEAD), BF16),
        ),
        in_specs=[any_spec, any_spec, smem, vmem],
        out_specs=(any_spec, vmem),
        scratch_shapes=[pltpu.VMEM((8, TILE, HEAD), BF16), pltpu.SMEM((1, 128), jnp.int32), dma],
        compiler_params=pltpu.CompilerParams(vmem_limit_bytes=16 * 2**20),
        name="unpack",
    )(
        landed.reshape(GROUPS, N_MP, LATE, TILE, HEAD),
        landed_early.reshape(N_MP, EARLY, GROUPS, TILE, HEAD),
        meta, states,
    )
    return packed.reshape(BLK_DEV * BLOCK, HEAD), state


def solution(mesh):
    in_specs = (
        P("dp", None),
        P(None, "mp"),
        P(),
        P("dp", None),
        P("dp", None),
        P("dp", None),
        P("dp", None),
    )
    out_specs = (P("dp", "mp"), P("dp", "mp"))
    return jax.shard_map(
        per_device, mesh=mesh, in_specs=in_specs, out_specs=out_specs, check_vma=False
    )
```

```python
import functools

import jax
import jax.numpy as jnp
from jax import lax
from jax.experimental import pallas as pl
from jax.experimental.pallas import tpu as pltpu
from jax.sharding import PartitionSpec as P

D = 512
HEADS = 4
HEAD = 128
BLOCK = 128
WINDOW = 256
USERS = 24
BLK_DEV = 48
N_DP = 64
N_MP = 4
OWN = USERS // N_MP
PARTS = (1, 2)
EARLY = sum(PARTS)
CHUNKS = len(PARTS)
STARTS = tuple(sum(PARTS[:c]) for c in range(CHUNKS))
LATE = OWN - EARLY
TILE = 16
GROUPS = WINDOW // TILE
EPS = 1e-05
MESH = pl.DeviceIdType.MESH
BF16 = jnp.bfloat16
F32 = jnp.float32


def shift_of(i):
    return 2 * (i % 2) + (i // 2) % 2


def gated_silu(v):
    half = v * 0.5
    return half + half * jnp.tanh(half)


def main_kernel(
    tokens, w_in, w_out, len_in, own_in, off_in, start_in,
    landed, landed_early, meta, states,
    tok, wbuf, wo, normed, att, gates, x_early, mix_early, tab, build, pin_v, pin_s, st_send, st_recv,
    len_v, own_v, off_v, len_s, own_s, start_s, out_late, mid_late, pack_late, *rest,
):
    out_early, mid_early, pack_early, in_early = (
        rest[n * CHUNKS : (n + 1) * CHUNKS] for n in range(4)
    )
    (loc_sem, tok_sem, in_sem, w_send, w_recv, f_send, f_recv, t_send, t_recv, s_send, s_recv,
    e1_send, e1_recv, e1_loc, e2_send, e2_recv, e2_loc, x_send, x_recv, x_loc,
    l1_send, l1_recv, l1_loc, l2_send, l2_recv, l2_loc, pin_sem) = rest[4 * CHUNKS :]
    me = lax.axis_index("dp")
    mp = lax.axis_index("mp")
    core = me % 2
    partner = me + 1 - 2 * core
    right = (mp + 1) % N_MP
    left = (mp + 3) % N_MP
    across = (mp + 2) % N_MP

    quarter = BLK_DEV // 4
    load_tok = [
        pltpu.make_async_copy(
            tokens.at[pl.ds(n * quarter, quarter)], tok.at[pl.ds(n * quarter, quarter)], tok_sem.at[n]
        )
        for n in range(4)
    ]
    small = [
        pltpu.make_async_copy(src, dst, in_sem.at[n])
        for n, (src, dst) in enumerate(
            (
                (start_in, start_s), (len_in, len_v), (own_in, own_v), (off_in, off_v),
                (len_in, len_s), (own_in, own_s),
            )
        )
    ]
    load_w = pltpu.make_async_copy(w_in, wbuf.at[mp], loc_sem.at[1])
    load_wo = pltpu.make_async_copy(w_out, wo, loc_sem.at[2])
    for copy in small:
        copy.start()
    for copy in load_tok:
        copy.start()
    load_w.start()
    load_wo.start()

    barrier = pltpu.get_barrier_semaphore()

    def greet(peer):
        pl.semaphore_signal(barrier, inc=1, device_id=(peer % N_DP, mp), device_id_type=MESH)

    greet(me + N_DP // 2)

    @pl.loop(1, N_DP // 2)
    def _(t):
        greet(me + N_DP // 2 + t)
        greet(me + N_DP // 2 - t)

    for other in (right, left, across):
        pl.semaphore_signal(barrier, inc=1, device_id=(me, other), device_id_type=MESH)

    for copy in small:
        copy.wait()

    build[...] = jnp.zeros_like(build)
    build[0:1, 0:USERS] = len_v[...]
    build[1:2, 0:USERS] = own_v[...]
    build[2:3, 0:USERS] = off_v[...]
    tab[me] = (
        build[0:1]
        + pltpu.roll(build[1:2], USERS, 1)
        + pltpu.roll(build[2:3], 2 * USERS, 1)
    )
    st_send[...] = jnp.zeros_like(st_send)

    for copy in load_tok:
        copy.wait()

    def user_blocks(k):
        start = start_s[0, mp * OWN + k]
        return tok[start], tok[jnp.minimum(start + 1, BLK_DEV - 1)]

    def user_rows(k):
        return jnp.concatenate(user_blocks(k), axis=0).astype(F32)

    for k in range(EARLY):
        for s, block in enumerate(user_blocks(k)):
            for q in range(N_MP):
                part = block[:, q * HEAD : (q + 1) * HEAD]
                c = sum(k >= low for low in STARTS) - 1
                out_early[c][q, s * 8 : s * 8 + 8, k - STARTS[c]] = part.reshape(8, TILE, HEAD)

    load_w.wait()
    pl.semaphore_wait(barrier, N_DP - 1 + N_MP - 1)

    half = pl.ds(pl.multiple_of(core * 256, 256), 256)

    def send_w(shard, target, k):
        return pltpu.make_async_remote_copy(
            src_ref=wbuf.at[shard, half], dst_ref=wbuf.at[shard, half],
            send_sem=w_send.at[k], recv_sem=w_recv.at[k],
            device_id=(me, target), device_id_type=MESH,
        )

    def forward_w(shard, k):
        return pltpu.make_async_remote_copy(
            src_ref=wbuf.at[shard, half], dst_ref=wbuf.at[shard, half],
            send_sem=f_send.at[k], recv_sem=f_recv.at[k],
            device_id=(partner, mp), device_id_type=MESH,
        )

    to_right = send_w(mp, right, 0)
    to_left = send_w(mp, left, 1)
    to_right.start()
    to_left.start()

    def send_tables():
        @pl.loop(1, N_DP)
        def _(t):
            pltpu.make_async_remote_copy(
                src_ref=tab.at[me], dst_ref=tab.at[me], send_sem=t_send, recv_sem=t_recv,
                device_id=((me + t) % N_DP, mp), device_id_type=MESH,
            ).start()

    own_early = []
    for c in range(CHUNKS):
        @pl.loop(1, N_DP)
        def _(t):
            i = (me + 27 * t) % N_DP
            pltpu.make_async_remote_copy(
                src_ref=out_early[c].at[i % 4, i // 4], dst_ref=mid_early[c].at[me],
                send_sem=e1_send.at[c], recv_sem=e1_recv.at[c],
                device_id=(i, mp), device_id_type=MESH,
            ).start()

        copy = pltpu.make_async_copy(
            out_early[c].at[me % 4, me // 4], mid_early[c].at[me], e1_loc.at[c]
        )
        copy.start()
        own_early.append(copy)
        if c == 0:
            send_tables()

    load_wo.wait()
    def normalize(k, x):
        mean = jnp.mean(x, axis=-1, keepdims=True)
        var = jnp.mean(x * x, axis=-1, keepdims=True) - mean * mean
        normed[k] = ((x - mean) * lax.rsqrt(var + EPS)).astype(BF16)

    @pl.loop(EARLY, OWN)
    def _(k):
        normalize(k, user_rows(k))

    row_id = lax.broadcasted_iota(jnp.int32, (BLOCK, BLOCK), 0)
    col_id = lax.broadcasted_iota(jnp.int32, (BLOCK, BLOCK), 1)
    causal = col_id <= row_id
    scaling = float(HEAD) ** -0.5
    nt = (((1,), (1,)), ((), ()))

    def head_of_user(shard, k):
        projected = gated_silu(
            jnp.dot(normed[k], wbuf[shard], preferred_element_type=F32)
        ).astype(BF16)
        gates[k, shard] = projected[:, 0:HEAD]
        v = projected[:, HEAD : 2 * HEAD]
        q = projected[:, 2 * HEAD : 3 * HEAD]
        key = projected[:, 3 * HEAD :]
        diag = jnp.concatenate(
            [
                lax.dot_general(q[:BLOCK], key[:BLOCK], nt, preferred_element_type=F32),
                lax.dot_general(q[BLOCK:], key[BLOCK:], nt, preferred_element_type=F32),
            ],
            axis=0,
        )
        back = lax.dot_general(q[BLOCK:], key[:BLOCK], nt, preferred_element_type=F32)
        both = jnp.concatenate([causal, causal], axis=0)
        w_diag = jnp.where(both, gated_silu(diag * scaling), 0.0).astype(BF16)
        w_back = gated_silu(back * scaling).astype(BF16)
        att[k, shard, 0:BLOCK] = jnp.dot(w_diag[:BLOCK], v[:BLOCK], preferred_element_type=F32)
        att[k, shard, BLOCK:] = jnp.dot(
            jnp.concatenate([w_back, w_diag[BLOCK:]], axis=1), v, preferred_element_type=F32
        )

    def heads(shard, low, high):
        @pl.loop(low, high)
        def _(k):
            head_of_user(shard, k)

    heads(mp, EARLY, OWN)

    def finish(k, x):
        a = [att[k, h] for h in range(HEADS)]
        total = sum(jnp.sum(p, axis=-1, keepdims=True) for p in a)
        squares = sum(jnp.sum(p * p, axis=-1, keepdims=True) for p in a)
        mean = total * (1.0 / D)
        var = squares * (1.0 / D) - mean * mean
        scale = lax.rsqrt(var + EPS * float(WINDOW * WINDOW))
        gated = jnp.concatenate(
            [((p - mean) * scale * gates[k, h].astype(F32)).astype(BF16) for h, p in enumerate(a)],
            axis=1,
        )
        mixed = jnp.dot(gated, wo[...], preferred_element_type=F32) + x
        return mixed

    def live_rows(mixed, count):
        rows = lax.broadcasted_iota(jnp.int32, (WINDOW, D), 0)
        return jnp.where(rows < count, mixed, 0.0).astype(BF16)

    def keep_state(k, mixed):
        last = len_s[0, mp * OWN + k] - 1
        rows = lax.broadcasted_iota(jnp.int32, (WINDOW, HEAD), 0)
        for q in range(N_MP):
            part = mixed[:, q * HEAD : (q + 1) * HEAD].astype(BF16).astype(F32)
            state = jnp.sum(jnp.where(rows == last, part, 0.0), axis=0, keepdims=True)
            st_send[q, pl.ds(k, 1)] = state

    to_right.wait_recv()
    from_left = forward_w(left, 0)
    from_left.start()
    to_left.wait_recv()
    from_right = forward_w(right, 1)
    from_right.start()
    onward_shard = jnp.where(core == 0, left, right)
    onward_target = jnp.where(core == 0, right, left)
    onward = send_w(onward_shard, onward_target, 2)
    onward.start()
    from_left.wait_recv()
    heads(left, EARLY, OWN)
    from_right.wait_recv()
    heads(right, EARLY, OWN)
    def wait_slots(ref, count, sem):
        some = ref.at[pl.ds(0, count)]
        pltpu.make_async_copy(some, some, sem).wait()

    wait_slots(tab, N_DP - 1, t_recv)
    rows = tab[...].reshape(N_DP, 128)
    owners = pltpu.roll(rows, 128 - USERS, 1)
    offsets = pltpu.roll(rows, 128 - 2 * USERS, 1)
    lane = lax.broadcasted_iota(jnp.int32, (N_DP, 128), 1)
    source = lax.broadcasted_iota(jnp.int32, (N_DP, 128), 0)

    def pick(mask, values):
        return jnp.max(jnp.where(mask, values, 0), axis=0, keepdims=True)

    pin = pick(owners[:, 0:1] == lane, source)
    lens = pick(owners == me, rows)
    offs = pick(owners == me, offsets)
    pin_v[...] = jnp.zeros((8, 128), jnp.int32)
    pin_v[0:1] = pin
    pin_v[1:2] = lens
    meta[...] = jnp.zeros((8, 128), jnp.int32)
    meta[0:1] = lens
    meta[1:2] = offs
    to_scalars = pltpu.make_async_copy(pin_v, pin_s, pin_sem)
    to_scalars.start()
    to_scalars.wait()

    def regroup(packed, middle, low, count):
        firsts = [own_s[0, low + j] - own_s[0, 0] for j in range(count)]

        @pl.loop(0, N_DP, unroll=4)
        def _(o):
            for j in range(count):
                packed[o, j] = middle[pin_s[0, (o - firsts[j]) & (N_DP - 1)], j]

    kept_early = []

    def second_of_early(c):
        wait_slots(mid_early[c], N_DP - 1, e1_recv.at[c])
        own_early[c].wait()
        regroup(pack_early[c], mid_early[c], mp * OWN + STARTS[c], PARTS[c])

        @pl.loop(1, N_DP)
        def _(t):
            o = (me + 27 * t) % N_DP
            pltpu.make_async_remote_copy(
                src_ref=pack_early[c].at[o], dst_ref=in_early[c].at[me],
                send_sem=e2_send.at[c], recv_sem=e2_recv.at[c],
                device_id=(o, mp), device_id_type=MESH,
            ).start()

        copy = pltpu.make_async_copy(pack_early[c].at[me], in_early[c].at[me], e2_loc.at[c])
        copy.start()
        kept_early.append(copy)

    onward.wait_recv()
    from_across = forward_w(across, 2)
    from_across.start()
    second_of_early(0)
    from_across.wait_recv()

    @pl.loop(0, LATE)
    def _(j):
        k = EARLY + j
        head_of_user(across, k)
        mixed = finish(k, user_rows(k))
        keep_state(k, mixed)
        mixed = live_rows(mixed, len_s[0, mp * OWN + k])
        for q in range(N_MP):
            part = mixed[:, q * HEAD : (q + 1) * HEAD]
            out_late[q, :, j] = part.reshape(GROUPS, TILE, HEAD)

    def send_late(i, hop):
        column = (mp + hop) % N_MP
        pltpu.make_async_remote_copy(
            src_ref=out_late.at[column, i // 4], dst_ref=mid_late.at[me],
            send_sem=l1_send, recv_sem=l1_recv,
            device_id=(i, column), device_id_type=MESH,
        ).start()

    @pl.loop(1, N_DP)
    def _(t):
        i = (me + 27 * t) % N_DP
        send_late(i, shift_of(i))

    hop = shift_of(me)

    @pl.when(hop != 0)
    def _():
        send_late(me, hop)

    @pl.when(hop == 0)
    def _():
        pltpu.make_async_copy(out_late.at[mp, me // 4], mid_late.at[me], l1_loc).start()

    for c in range(1, CHUNKS):
        second_of_early(c)

    @pl.loop(0, EARLY)
    def _(k):
        normalize(k, user_rows(k))

    for shard in (mp, left, right):
        heads(shard, 0, EARLY)

    @pl.loop(0, EARLY)
    def _(k):
        head_of_user(across, k)
        keep_state(k, finish(k, user_rows(k)))

    state_copies = []
    for n, (other, source) in enumerate(((right, left), (left, right), (across, across))):
        copy = pltpu.make_async_remote_copy(
            src_ref=st_send.at[other], dst_ref=st_recv.at[mp],
            send_sem=s_send.at[n], recv_sem=s_recv.at[n],
            device_id=(me, other), device_id_type=MESH,
        )
        copy.start()
        state_copies.append(copy)

    @pl.when(hop != 0)
    def _():
        wait_slots(mid_late, N_DP, l1_recv)

    @pl.when(hop == 0)
    def _():
        wait_slots(mid_late, N_DP - 1, l1_recv)
        pltpu.make_async_copy(out_late.at[mp, me // 4], mid_late.at[me], l1_loc).wait()

    regroup(pack_late, mid_late, (mp - hop + N_MP) % N_MP * OWN + EARLY, LATE)

    @pl.loop(1, N_DP)
    def _(t):
        o = (me + 27 * t) % N_DP
        pltpu.make_async_remote_copy(
            src_ref=pack_late.at[o], dst_ref=landed.at[me],
            send_sem=l2_send, recv_sem=l2_recv,
            device_id=(o, mp), device_id_type=MESH,
        ).start()

    kept_late = pltpu.make_async_copy(pack_late.at[me], landed.at[me], l2_loc)
    kept_late.start()

    for c in range(CHUNKS):
        wait_slots(in_early[c], N_DP - 1, e2_recv.at[c])
        kept_early[c].wait()
        mine = range(STARTS[c], STARTS[c] + PARTS[c])

        @pl.loop(0, GROUPS)
        def _(g):
            rows = pl.ds(pl.multiple_of(g * TILE, TILE), TILE)
            for q in range(N_MP):
                for k in mine:
                    x_early[k, rows, q * HEAD : (q + 1) * HEAD] = in_early[c][4 * g + q, k - STARTS[c]]

        for k in mine:
            normalize(k, x_early[k].astype(F32))

        for shard in (mp, left, right):
            heads(shard, mine[0], mine[0] + PARTS[c])

        @pl.loop(mine[0], mine[0] + PARTS[c])
        def _(k):
            head_of_user(across, k)
            mixed = live_rows(finish(k, x_early[k].astype(F32)), pin_s[1, mp * OWN + k])
            for q in range(N_MP):
                mix_early[q, k] = mixed[:, q * HEAD : (q + 1) * HEAD]
            for n, other in enumerate((right, left, across)):
                pltpu.make_async_remote_copy(
                    src_ref=mix_early.at[other, k], dst_ref=landed_early.at[mp, k],
                    send_sem=x_send.at[n], recv_sem=x_recv.at[n],
                    device_id=(me, other), device_id_type=MESH,
                ).start()

    kept = pltpu.make_async_copy(mix_early.at[mp], landed_early.at[mp], x_loc)
    kept.start()

    for copy in state_copies:
        copy.wait()
    for m in range(N_MP):
        @pl.when(m != mp)
        def _():
            states[m] = st_recv[m]

        @pl.when(m == mp)
        def _():
            states[m] = st_send[m]

    for copy in (to_right, to_left, onward, from_left, from_right, from_across):
        copy.wait_send()
    wait_slots(tab, N_DP - 1, t_send)
    for c in range(CHUNKS):
        wait_slots(mid_early[c], N_DP - 1, e1_send.at[c])
        wait_slots(mid_early[c], N_DP - 1, e2_send.at[c])

    @pl.when(hop != 0)
    def _():
        wait_slots(mid_late, N_DP, l1_send)

    @pl.when(hop == 0)
    def _():
        wait_slots(mid_late, N_DP - 1, l1_send)

    wait_slots(mid_late, N_DP - 1, l2_send)
    for n, (other, source) in enumerate(((right, left), (left, right), (across, across))):
        pltpu.make_async_remote_copy(
            src_ref=mix_early.at[other], dst_ref=landed_early.at[source],
            send_sem=x_send.at[n], recv_sem=x_recv.at[n],
            device_id=(me, other), device_id_type=MESH,
        ).wait()
    kept.wait()

    wait_slots(mid_late, N_DP - 1, l2_recv)
    kept_late.wait()


def unpack_kernel(landed, landed_early, meta, states, out, state_out, zeros, block_of, sem):
    mp = lax.axis_index("mp")
    zeros[...] = jnp.zeros_like(zeros)

    @pl.loop(0, BLK_DEV, unroll=8)
    def _(b):
        block_of[0, b] = -1

    for m in range(N_MP):
        for k in range(OWN):
            u = m * OWN + k
            code = (m * 8 + k) * 2
            first = meta[1, u]
            block_of[0, first] = code

            @pl.when(meta[0, u] > BLOCK)
            def _():
                block_of[0, first + 1] = code + 1

    @pl.loop(0, BLK_DEV)
    def _(b):
        code = block_of[0, b]
        m = (code >> 4) & 3
        k = (code >> 1) & 7
        groups = pl.ds((code & 1) * 8, 8)

        @pl.when(code < 0)
        def _():
            pltpu.make_async_copy(zeros, out.at[b], sem).start()

        @pl.when((code >= 0) & (k < EARLY))
        def _():
            pltpu.make_async_copy(landed_early.at[m, k, groups], out.at[b], sem).start()

        @pl.when((code >= 0) & (k >= EARLY))
        def _():
            delta = (mp - m) & 3
            low = (delta >> 1) + 2 * (delta & 1)
            pltpu.make_async_copy(landed.at[groups, low, k - EARLY], out.at[b], sem).start()

    for m in range(N_MP):
        for k in range(OWN):
            state_out[pl.ds(m * OWN + k, 1)] = states[m, pl.ds(k, 1)].astype(BF16)
    pltpu.make_async_copy(out, out, sem).wait()


def per_device(tokens, w_uvqk, w_out, hist_len, owner, recv_offset, block_start):
    any_spec = pl.BlockSpec(memory_space=pl.ANY)
    vmem = pl.BlockSpec(memory_space=pltpu.VMEM)
    smem = pl.BlockSpec(memory_space=pltpu.SMEM)
    dma = pltpu.SemaphoreType.DMA
    landed, landed_early, meta, states = pl.pallas_call(
        main_kernel,
        out_shape=(
            jax.ShapeDtypeStruct((N_DP, LATE, TILE, HEAD), BF16),
            jax.ShapeDtypeStruct((N_MP, EARLY, WINDOW, HEAD), BF16),
            jax.ShapeDtypeStruct((8, 128), jnp.int32),
            jax.ShapeDtypeStruct((N_MP, 8, HEAD), F32),
        ),
        in_specs=[any_spec] * 7,
        out_specs=(any_spec, any_spec, vmem, vmem),
        scratch_shapes=[
            pltpu.VMEM((BLK_DEV, BLOCK, D), BF16),
            pltpu.VMEM((N_MP, D, D), BF16),
            pltpu.VMEM((D, D), BF16),
            pltpu.VMEM((OWN, WINDOW, D), BF16),
            pltpu.VMEM((OWN, HEADS, WINDOW, HEAD), F32),
            pltpu.VMEM((OWN, HEADS, WINDOW, HEAD), BF16),
            pltpu.VMEM((EARLY, WINDOW, D), BF16),
            pltpu.VMEM((N_MP, EARLY, WINDOW, HEAD), BF16),
            pltpu.VMEM((N_DP, 1, 128), jnp.int32),
            pltpu.VMEM((8, 128), jnp.int32),
            pltpu.VMEM((8, 128), jnp.int32),
            pltpu.SMEM((8, 128), jnp.int32),
            pltpu.VMEM((N_MP, 8, HEAD), F32),
            pltpu.VMEM((N_MP, 8, HEAD), F32),
            *[pltpu.VMEM((1, USERS), jnp.int32)] * 3,
            *[pltpu.SMEM((1, USERS), jnp.int32)] * 3,
            pltpu.VMEM((N_MP, GROUPS, LATE, TILE, HEAD), BF16),
            pltpu.VMEM((N_DP, LATE, TILE, HEAD), BF16),
            pltpu.VMEM((N_DP, LATE, TILE, HEAD), BF16),
        ]
        + [pltpu.VMEM((N_MP, GROUPS, part, TILE, HEAD), BF16) for part in PARTS]
        + [pltpu.VMEM((N_DP, part, TILE, HEAD), BF16) for part in PARTS * 3]
        + [
            dma((3,)), dma((4,)), dma((6,)), dma((3,)), dma((3,)), dma((3,)), dma((3,)), dma, dma, dma((3,)), dma((3,)),
            *[dma((CHUNKS,))] * 6, dma((3,)), dma((3,)), dma,
            dma, dma, dma, dma, dma, dma, dma,
        ],
        compiler_params=pltpu.CompilerParams(
            collective_id=0, has_side_effects=True, vmem_limit_bytes=40 * 2**20
        ),
        name="layer_and_repack",
    )(
        *(
            pltpu.with_memory_space_constraint(a, pltpu.HBM)
            for a in (
                tokens.reshape(BLK_DEV, BLOCK, D), w_uvqk, w_out,
                hist_len, owner, recv_offset, block_start,
            )
        )
    )
    packed, state = pl.pallas_call(
        unpack_kernel,
        out_shape=(
            jax.ShapeDtypeStruct((BLK_DEV, 8, TILE, HEAD), BF16),
            jax.ShapeDtypeStruct((USERS, HEAD), BF16),
        ),
        in_specs=[any_spec, any_spec, smem, vmem],
        out_specs=(any_spec, vmem),
        scratch_shapes=[pltpu.VMEM((8, TILE, HEAD), BF16), pltpu.SMEM((1, 128), jnp.int32), dma],
        compiler_params=pltpu.CompilerParams(vmem_limit_bytes=16 * 2**20),
        name="unpack",
    )(
        landed.reshape(GROUPS, N_MP, LATE, TILE, HEAD),
        landed_early.reshape(N_MP, EARLY, GROUPS, TILE, HEAD),
        meta, states,
    )
    return packed.reshape(BLK_DEV * BLOCK, HEAD), state


def solution(mesh):
    in_specs = (
        P("dp", None),
        P(None, "mp"),
        P(),
        P("dp", None),
        P("dp", None),
        P("dp", None),
        P("dp", None),
    )
    out_specs = (P("dp", "mp"), P("dp", "mp"))
    return jax.shard_map(
        per_device, mesh=mesh, in_specs=in_specs, out_specs=out_specs, check_vma=False
    )
```
